32 devices in a mesh: dp: 8 (over y, x, core), blk: 4 (over z).
Axes of the slice: x: 2, y: 2, z: 4, core: 2. Of those that a mesh axis runs over, the one named last changes fastest.
Arguments:
- layer_input: bfloat16 [8, 1024, 2048], P('dp', 'blk'), may hold values from -6 to 6
- queries: bfloat16 [8, 1024, 1024], P('dp', 'blk'), may hold values from -28 to 28
- key_rows: bfloat16 [8, 1024, 1024], P('dp', 'blk'), may hold values from -4 to 4
- value_rows: bfloat16 [8, 1024, 1024], P('dp', 'blk'), may hold values from -6 to 6
- context: bfloat16 [8, 1024, 1024], P('dp', 'blk'), may hold values from -6 to 6
- grad_context: bfloat16 [8, 1024, 1024], P('dp', 'blk'), may hold values from -6 to 6
- grad_output: bfloat16 [8, 1024, 2048], P('dp', 'blk'), may hold values from -6 to 6
- earlier_mass: float32 [8, 4, 1024], P('dp', None, 'blk'), may hold values from 3 to 7
- grad_queries: float32 [8, 1024, 1024], P('dp', 'blk'), may hold values from -0.12 to 0.12
- grad_keys: float32 [8, 1024, 1024], P('dp', 'blk'), may hold values from -0.12 to 0.12
- grad_values: float32 [8, 1024, 1024], P('dp', 'blk'), may hold values from -0.12 to 0.12
- documents: int32 [8, 1024], P('dp', 'blk'), may hold values from 0 to 2, as said below
- weights: float32 [4, 2048, 1024], P(None, 'blk', 'dp'), may hold values from -0.125 to 0.125
- row_factor: float32 [4, 2048], P(None, 'blk'), may hold values from 1.2207032e-07 to 0.00012207031
- column_factor: float32 [4, 1024], P(None, 'dp'), may hold values from 1.2207032e-07 to 0.00012207031
Outputs:
- new_weights: float32 [4, 2048, 1024], P(None, 'blk', 'dp')
- new_row_factor: float32 [4, 2048], P(None, 'blk')
- new_column_factor: float32 [4, 1024], P(None, 'dp')
The draws below stay inside these ranges and needn't reach their ends.
Inputs may be any that keep to these rules, and one draw needn't show every extreme that they name: Read in order of position, a sequence's document numbers never fall; each sequence has three documents of 128 positions or more.
All inputs are finite; a program needn't handle non-finite values.
Results may differ from the reference program's by a relative error of at most 0.022.
Values may be sent and summed in bfloat16 or wider, within the bound.
No kernel may reach another device: no remote copies, remote signals or barrier semaphores. Data moves between devices by JAX's collectives and lax.ppermute only.
A program may use at most 128 MiB of HBM per device.

```python
import math
import jax
import jax.numpy as jnp
from jax import lax

D = 2048
H = 4
TOK_DEV = 256
HH = 1024
LEN = 1024
BATCH = 8
N_BLK = 4


def folded_order(blocks, row_count):
    half = row_count // 2
    block_ids = jnp.arange(blocks, dtype=jnp.int32)[:, None]
    local = jnp.arange(row_count, dtype=jnp.int32)[None, :]
    lower = block_ids * half + local
    upper = (2 * blocks - 1 - block_ids) * half + local - half
    return jnp.where(local < half, lower, upper).reshape(-1)


def draw_documents(key, part):
    blocks = LEN // TOK_DEV
    order = folded_order(blocks, TOK_DEV)
    first_cut = jax.random.randint(jax.random.fold_in(key, 11), (BATCH, 1), LEN // 8, LEN // 2)
    second_cut = jax.random.randint(jax.random.fold_in(key, 12), (BATCH, 1), LEN // 2 + LEN // 8, LEN - LEN // 8 + 1)
    return (order[None, :] >= first_cut).astype(jnp.int32) + (order[None, :] >= second_cut).astype(jnp.int32)


def draw_pair(key):
    key_draw = jnp.clip(jax.random.normal(jax.random.fold_in(key, 21), (BATCH, LEN, HH), jnp.float32), -4.0, 4.0)
    query_draw = jnp.clip(jax.random.normal(jax.random.fold_in(key, 22), (BATCH, LEN, HH), jnp.float32), -4.0, 4.0)
    return (key_draw, query_draw)


def draw_key_rows(key, part):
    return draw_pair(key)[0].astype(jnp.bfloat16)


def draw_queries(key, part):
    return draw_pair(key)[1].astype(jnp.bfloat16)


def spiked(array, key, source, target, blocks, factor):
    def block_of(position):
        return (jnp.arange(array.shape[position]) // (array.shape[position] // blocks)).reshape((-1,) + (1,) * (array.ndim - 1 - position))

    near = jax.random.permutation(key, blocks)[block_of(target)]
    far = (block_of(target) + blocks // 2) % blocks
    return jnp.where((block_of(source) == near) | (block_of(source) == far), factor * array, array)


def shard_levels(key, extent, shards, least, largest):
    def one(position, shards_of):
        draws = jax.random.uniform(jax.random.fold_in(jax.random.fold_in(key, 6), position), (shards_of,), jnp.float32, least / len(shards), largest / len(shards))
        return jnp.repeat(jnp.exp(draws), extent[position] // shards_of).reshape((-1,) + (1,) * (len(extent) - position - 1))

    loudness = one(*shards[0])
    for cut in shards[1:]:
        loudness = loudness * one(*cut)
    return loudness


def centred(key, shape, spread, reach, split=(), held_as=jnp.bfloat16):
    array = spread * jax.random.normal(key, shape, jnp.float32)
    if split:
        array = array * shard_levels(key, shape, split, -0.22, 0.18)
    return jnp.clip(array, -reach, reach).astype(held_as)


def heavy_noise(key, dims, width, bound, split, heavy, held_as=jnp.bfloat16):
    result = width * jax.random.normal(key, dims, jnp.float32)
    if split:
        result = result * shard_levels(key, dims, split, -0.22, 0.18)
    return jnp.clip(spiked(result, jax.random.fold_in(key, 3), *heavy), -bound, bound).astype(held_as)


def setup_inputs(seed: int = 0) -> dict:
    arg_keys = jax.random.split(jax.random.key(seed), 16)
    layer_input = heavy_noise(arg_keys[0], (BATCH, LEN, D), 1.0, 6.0, ((0, 8), (1, 4)), (1, 2, 4, 2.0))
    queries = draw_queries(jax.random.fold_in(arg_keys[15], 71), 0)
    key_rows = draw_key_rows(jax.random.fold_in(arg_keys[15], 71), 0)
    value_rows = centred(arg_keys[3], (BATCH, LEN, HH), 1.0, 6.0, ((0, 8), (1, 4)))
    context = centred(arg_keys[4], (BATCH, LEN, HH), 1.0, 6.0, ((0, 8), (1, 4)))
    grad_context = centred(arg_keys[5], (BATCH, LEN, HH), 1.0, 6.0, ((0, 8), (1, 4)))
    grad_output = heavy_noise(arg_keys[6], (BATCH, LEN, D), 1.0, 6.0, ((0, 8), (1, 4)), (1, 2, 4, 2.0))
    earlier_mass = jnp.clip(3.0 + 4.0 * jax.random.uniform(arg_keys[7], (BATCH, H, LEN), jnp.float32) ** shard_levels(arg_keys[7], (BATCH, H, LEN), ((0, 8), (2, 4)), -0.2, 0.2), 3.0, 7.0)
    grad_queries = heavy_noise(arg_keys[8], (BATCH, LEN, HH), 0.02, 0.12, ((0, 8), (1, 4)), (0, 2, 8, 2.0), jnp.float32)
    grad_keys = centred(arg_keys[9], (BATCH, LEN, HH), 0.02, 0.12, ((0, 8), (1, 4)), jnp.float32)
    grad_values = centred(arg_keys[10], (BATCH, LEN, HH), 0.02, 0.12, ((0, 8), (1, 4)), jnp.float32)
    documents = draw_documents(jax.random.fold_in(arg_keys[15], 71), 0)
    weights = centred(arg_keys[12], (4, D, HH), D ** -0.5, 0.125, ((1, 4), (2, 8)), jnp.float32)
    row_factor = jnp.clip(jnp.exp(math.log(0.00012207031) - 6.9077552 * jax.random.uniform(arg_keys[13], (4, D), jnp.float32) ** shard_levels(arg_keys[13], (4, D), ((1, 4),), -0.2, 0.2)), 1.2207031829802872e-07, 0.00012207031)
    column_factor = jnp.clip(jnp.exp(math.log(0.00012207031) - 6.9077552 * jax.random.uniform(arg_keys[14], (4, HH), jnp.float32) ** shard_levels(arg_keys[14], (4, HH), ((1, 8),), -0.2, 0.2)), 1.2207031829802872e-07, 0.00012207031)
    return {"layer_input": layer_input, "queries": queries, "key_rows": key_rows, "value_rows": value_rows, "context": context, "grad_context": grad_context, "grad_output": grad_output, "earlier_mass": earlier_mass, "grad_queries": grad_queries, "grad_keys": grad_keys, "grad_values": grad_values, "documents": documents, "weights": weights, "row_factor": row_factor, "column_factor": column_factor}


beta_two = 0.9
learn_rate = 0.05
tiny_square = 1e-30
exact = lax.Precision.HIGHEST

def folded_table(blocks, row_count):
    half = row_count // 2
    block_ids = jnp.arange(blocks, dtype=jnp.int32)[:, None]
    local = jnp.arange(row_count, dtype=jnp.int32)[None, :]
    lower = block_ids * half + local
    upper = (2 * blocks - 1 - block_ids) * half + local - half
    return jnp.where(local < half, lower, upper)

def attend_back(queries, key_rows, value_rows, context, grad_context, earlier_mass, allowed):
    row_count = queries.shape[0]
    key_count = key_rows.shape[0]
    head_count = earlier_mass.shape[0]
    head_size = queries.shape[1] // head_count
    scale_factor = 1.0 / math.sqrt(head_size)
    query_heads = queries.astype(jnp.float32).reshape(row_count, head_count, head_size)
    key_heads = key_rows.astype(jnp.float32).reshape(key_count, head_count, head_size)
    value_heads = value_rows.astype(jnp.float32).reshape(key_count, head_count, head_size)
    context_heads = context.astype(jnp.float32).reshape(row_count, head_count, head_size)
    grad_heads = grad_context.astype(jnp.float32).reshape(row_count, head_count, head_size)
    scores = jnp.einsum('thd,shd->hts', query_heads, key_heads, precision=exact) * scale_factor
    open_pairs = allowed[None]
    peak_score = jnp.maximum(earlier_mass, lax.optimization_barrier(jnp.max(jnp.where(open_pairs, scores, -jnp.inf), axis=2)))
    shifted = jnp.where(open_pairs, jnp.exp(scores - peak_score[:, :, None]), 0.0)
    total_mass = jnp.exp(earlier_mass - peak_score) + lax.optimization_barrier(jnp.sum(shifted, axis=2))
    log_norm = peak_score + jnp.log(total_mass)
    attention = jnp.where(open_pairs, jnp.exp(scores - log_norm[:, :, None]), 0.0)
    attention_low = attention.astype(jnp.bfloat16).astype(jnp.float32)
    row_dot = lax.optimization_barrier(jnp.sum(context_heads * grad_heads, axis=2)).T
    grad_attention = jnp.einsum('thd,shd->hts', grad_heads, value_heads, precision=exact)
    grad_scores = (attention * (grad_attention - row_dot[:, :, None]) * scale_factor).astype(jnp.bfloat16).astype(jnp.float32)
    query_step = jnp.einsum('hts,shd->thd', grad_scores, key_heads, precision=exact).reshape(row_count, -1)
    key_step = jnp.einsum('hts,thd->shd', grad_scores, query_heads, precision=exact).reshape(key_count, -1)
    value_step = jnp.einsum('hts,thd->shd', attention_low, grad_heads, precision=exact).reshape(key_count, -1)
    return (query_step, key_step, value_step)

def reference(layer_input, queries, key_rows, value_rows, context, grad_context, grad_output, earlier_mass, grad_queries, grad_keys, grad_values, documents, weights, row_factor, column_factor):
    blocks = N_BLK
    row_count = TOK_DEV
    positions = folded_table(blocks, row_count)
    seen_pos = jnp.concatenate([jnp.roll(positions, -1, axis=0), jnp.roll(positions, -2, axis=0)], axis=1)
    causal = seen_pos[:, None, :] <= positions[:, :, None]

    def visited(blocked):
        return jnp.concatenate([jnp.roll(blocked, -1, axis=0), jnp.roll(blocked, -2, axis=0)], axis=1)

    def one_sequence(items):
        query_seq, key_seq, value_seq, context_seq, grad_seq, mass_seq, doc_seq = items
        query_blocks = query_seq.reshape(blocks, row_count, -1)
        key_seen = visited(key_seq.reshape(blocks, row_count, -1))
        value_seen = visited(value_seq.reshape(blocks, row_count, -1))
        context_blocks = context_seq.reshape(blocks, row_count, -1)
        grad_blocks = grad_seq.reshape(blocks, row_count, -1)
        doc_blocks = doc_seq.reshape(blocks, row_count)
        doc_seen = visited(doc_blocks)
        allowed = causal & (doc_seen[:, None, :] == doc_blocks[:, :, None])
        mass_blocks = jnp.transpose(mass_seq.reshape(mass_seq.shape[0], blocks, row_count), (1, 0, 2))
        query_step, key_step, value_step = jax.vmap(attend_back)(query_blocks, key_seen, value_seen, context_blocks, grad_blocks, mass_blocks, allowed)
        key_home = jnp.roll(key_step[:, :row_count], 1, axis=0) + jnp.roll(key_step[:, row_count:], 2, axis=0)
        value_home = jnp.roll(value_step[:, :row_count], 1, axis=0) + jnp.roll(value_step[:, row_count:], 2, axis=0)
        return (query_step.reshape(LEN, -1), key_home.reshape(LEN, -1), value_home.reshape(LEN, -1))
    query_add, key_add, value_add = lax.map(one_sequence, (queries, key_rows, value_rows, context, grad_context, earlier_mass, documents))
    query_total = grad_queries + query_add
    key_total = grad_keys + key_add
    value_total = grad_values + value_add
    units = BATCH * blocks
    right_low = jnp.stack([query_total, key_total, value_total], axis=2).astype(jnp.bfloat16).reshape(units, row_count, 3, HH)
    left_units = layer_input.reshape(units, row_count, D)
    outer_units = grad_output.reshape(units, row_count, D)
    inner_units = context.reshape(units, row_count, HH)

    def add_unit(total, unit):
        left_part, right_part, outer_part, inner_part = unit
        part_inner = jnp.einsum('td,twh->dwh', left_part.astype(jnp.float32), right_part.astype(jnp.float32), precision=exact)
        part_output = jnp.einsum('td,th->dh', outer_part.astype(jnp.float32), inner_part.astype(jnp.float32), precision=exact)
        partial_value = jnp.concatenate([part_inner, part_output[:, None, :]], axis=1)
        rounded = lax.optimization_barrier(partial_value.astype(jnp.bfloat16))
        return (total + rounded.astype(jnp.float32), None)
    total, unused = lax.scan(add_unit, jnp.zeros((D, 4, HH), jnp.float32), (left_units, right_low, outer_units, inner_units))
    gradient = jnp.transpose(total, (1, 0, 2)) / (BATCH * LEN)
    squares = gradient * gradient + tiny_square
    new_row_factor = beta_two * row_factor + (1.0 - beta_two) * lax.optimization_barrier(jnp.mean(squares, axis=2))
    new_column_factor = beta_two * column_factor + (1.0 - beta_two) * lax.optimization_barrier(jnp.mean(squares, axis=1))
    row_mean = lax.optimization_barrier(jnp.mean(new_row_factor, axis=1))
    second = new_row_factor[:, :, None] * new_column_factor[:, None, :] / row_mean[:, None, None]
    new_weights = weights - learn_rate * gradient * lax.rsqrt(second)
    return (new_weights, new_row_factor, new_column_factor)
```

```python
import math

import jax
import jax.numpy as jnp
from jax import lax
from jax.experimental import pallas as pl
from jax.experimental.pallas import tpu as pltpu
from jax.sharding import PartitionSpec as P

beta_two = 0.9
learn_rate = 0.05
tiny_square = 1e-30


def passed_along(value, axis, steps):
    count = lax.axis_size(axis)
    pairs = [(source, (source + steps) % count) for source in range(count)]
    return lax.ppermute(value, axis, pairs)


def as_sent(array):
    return jax.tree.map(lambda a: a.astype(jnp.bfloat16) if a.dtype == jnp.float32 else a, array)


def folded_rows(block_index, blocks, row_count):
    half = row_count // 2
    local = jnp.arange(row_count, dtype=jnp.int32)
    lower = block_index * half + local
    upper = (2 * blocks - 1 - block_index) * half + local - half
    return jnp.where(local < half, lower, upper)


def attend_back(queries, key_rows, value_rows, context, grad_context, earlier_mass, allowed):
    row_count = queries.shape[0]
    key_count = key_rows.shape[0]
    head_count = earlier_mass.shape[0]
    head_size = queries.shape[1] // head_count
    scale_factor = 1.0 / math.sqrt(head_size)
    query_heads = queries.reshape(row_count, head_count, head_size)
    key_heads = key_rows.reshape(key_count, head_count, head_size)
    value_heads = value_rows.reshape(key_count, head_count, head_size)
    context_heads = context.reshape(row_count, head_count, head_size)
    grad_heads = grad_context.reshape(row_count, head_count, head_size)
    scores = (
        jnp.einsum("thd,shd->hts", query_heads, key_heads, preferred_element_type=jnp.float32)
        * scale_factor
    )
    open_pairs = allowed[None]
    peak_score = jnp.maximum(earlier_mass, jnp.max(jnp.where(open_pairs, scores, -jnp.inf), axis=2))
    shifted = jnp.where(open_pairs, jnp.exp(scores - peak_score[:, :, None]), 0.0)
    total_mass = jnp.exp(earlier_mass - peak_score) + jnp.sum(shifted, axis=2)
    log_norm = peak_score + jnp.log(total_mass)
    attention = jnp.where(open_pairs, jnp.exp(scores - log_norm[:, :, None]), 0.0)
    attention_low = attention.astype(jnp.bfloat16)
    row_dot = jnp.sum(context_heads.astype(jnp.float32) * grad_heads.astype(jnp.float32), axis=2).T
    grad_attention = jnp.einsum(
        "thd,shd->hts", grad_heads, value_heads, preferred_element_type=jnp.float32
    )
    grad_scores = (attention * (grad_attention - row_dot[:, :, None]) * scale_factor).astype(
        jnp.bfloat16
    )
    query_step = jnp.einsum(
        "hts,shd->thd", grad_scores, key_heads, preferred_element_type=jnp.float32
    ).reshape(row_count, -1)
    key_step = jnp.einsum(
        "hts,thd->shd", grad_scores, query_heads, preferred_element_type=jnp.float32
    ).reshape(key_count, -1)
    value_step = jnp.einsum(
        "hts,thd->shd", attention_low, grad_heads, preferred_element_type=jnp.float32
    ).reshape(key_count, -1)
    return (query_step, key_step, value_step)


def ring_body(
    layer_input,
    queries,
    key_rows,
    value_rows,
    context,
    grad_context,
    grad_output,
    earlier_mass,
    grad_queries,
    grad_keys,
    grad_values,
    documents,
    weights,
    row_factor,
    column_factor,
):
    blocks = lax.axis_size("blk")
    data_count = lax.axis_size("dp")
    block_index = lax.axis_index("blk")
    row_count = queries.shape[1]
    own_docs = documents[0]
    doc_float = own_docs.astype(jnp.bfloat16)

    def fetch_next(held):
        return passed_along((held[0], held[1], held[2]), "blk", -1)

    nearer = fetch_next((key_rows[0], value_rows[0], doc_float))
    further = fetch_next(nearer)
    seen_keys = jnp.concatenate([nearer[0], further[0]], axis=0)
    seen_values = jnp.concatenate([nearer[1], further[1]], axis=0)
    seen_docs = jnp.concatenate([nearer[2], further[2]], axis=0).astype(jnp.int32)
    own_pos = folded_rows(block_index, blocks, row_count)
    near_pos = folded_rows((block_index + 1) % blocks, blocks, row_count)
    far_pos = folded_rows((block_index + 2) % blocks, blocks, row_count)
    seen_pos = jnp.concatenate([near_pos, far_pos], axis=0)
    allowed = (seen_pos[None, :] <= own_pos[:, None]) & (seen_docs[None, :] == own_docs[:, None])
    query_step, key_step, value_step = attend_back(
        queries[0], seen_keys, seen_values, context[0], grad_context[0], earlier_mass[0], allowed
    )
    near_part = (key_step[:row_count], value_step[:row_count])
    far_part = (key_step[row_count:], value_step[row_count:])

    def send_back(pair):
        return passed_along((as_sent(pair[0]), as_sent(pair[1])), "blk", 1)

    moved = send_back(far_part)
    home = send_back((moved[0] + near_part[0], moved[1] + near_part[1]))
    query_total = grad_queries[0] + query_step
    key_total = grad_keys[0] + home[0]
    value_total = grad_values[0] + home[1]
    right_low = jnp.stack([query_total, key_total, value_total], axis=1).astype(jnp.bfloat16)
    layer_rows = layer_input[0]
    output_rows = grad_output[0]
    context_rows = context[0]
    all_tokens = data_count * blocks * row_count
    part_inner = jnp.einsum(
        "twh,td->hwd", right_low, layer_rows, preferred_element_type=jnp.float32
    )
    part_output = jnp.einsum(
        "th,td->hd", context_rows, output_rows, preferred_element_type=jnp.float32
    )
    summed = lax.psum_scatter(
        jnp.concatenate([part_inner, part_output[:, None, :]], axis=1).astype(jnp.bfloat16),
        "dp",
        scatter_dimension=0,
        tiled=True,
    )
    grouped = lax.psum_scatter(summed, "blk", scatter_dimension=2, tiled=True).astype(jnp.float32)
    gradient = jnp.transpose(grouped, (1, 2, 0)) / all_tokens
    local_rows = gradient.shape[1]
    local_cols = gradient.shape[2]
    full_rows = local_rows * blocks
    full_cols = local_cols * data_count
    squares = gradient * gradient + tiny_square
    row_part = jnp.sum(squares, axis=2)
    col_part = jnp.sum(squares, axis=1)
    row_sum = lax.psum(row_part, "dp")
    col_sum = lax.psum(col_part, "blk")
    new_row_factor = beta_two * row_factor + (1.0 - beta_two) * row_sum / full_cols
    new_column_factor = beta_two * column_factor + (1.0 - beta_two) * col_sum / full_rows
    row_mean = lax.psum(jnp.sum(new_row_factor, axis=1), "blk") / full_rows
    second = new_row_factor[:, :, None] * new_column_factor[:, None, :] / row_mean[:, None, None]
    new_weights = weights - learn_rate * gradient * lax.rsqrt(second)
    return (new_weights, new_row_factor, new_column_factor)


def swapped(value, mask):
    count = lax.axis_size("dp")
    return lax.ppermute(value, "dp", [(source, source ^ mask) for source in range(count)])


def rotated(value, steps):
    count = lax.axis_size("blk")
    return lax.ppermute(value, "blk", [(source, (source + steps) % count) for source in range(count)])


def head_kernel(blocks, groups, block_ref, *refs):
    packs = refs[:blocks]
    sides = refs[blocks : 2 * blocks]
    outs = refs[2 * blocks : -2]
    weight_ref, slope_ref = refs[-2:]
    rows = packs[0].shape[1]
    half = rows // 2
    scale_factor = 1.0 / math.sqrt(packs[0].shape[2])
    local_down = lax.broadcasted_iota(jnp.int32, (rows, 1), 0)
    local_across = lax.broadcasted_iota(jnp.int32, (1, rows), 1)
    block_of = [lax.rem(block_ref[0] + step, blocks) for step in range(blocks)]

    def positions(local, block):
        lower = block * half + local
        upper = (2 * blocks - 1 - block) * half + local - half
        return jnp.where(local < half, lower, upper)

    def times(left, right, left_dim, right_dim):
        return lax.dot_general(
            left,
            right,
            (((left_dim,), (right_dim,)), ((), ())),
            preferred_element_type=jnp.float32,
        )

    for step in range(blocks):
        visited = [(step + 1) % blocks, (step + 2) % blocks]
        side = sides[step][...].T
        mass, row_dot, docs = side[:, 0:1], side[:, 1:2], side[:, 2:3]
        own_pos = positions(local_down, block_of[step])
        scored = []
        for other in visited:
            score = times(packs[step][0], packs[other][1], 1, 1) * scale_factor
            allowed = (positions(local_across, block_of[other]) <= own_pos) & (
                sides[other][2:3, :] == docs
            )
            scored.append(jnp.where(allowed, score, -jnp.inf))
        peak = mass
        for score in scored:
            peak = jnp.maximum(peak, jnp.max(score, axis=1, keepdims=True))
        shifted = [jnp.exp(score - peak) for score in scored]
        total = jnp.exp(mass - peak)
        for part in shifted:
            total = total + jnp.sum(part, axis=1, keepdims=True)
        inverse = 1.0 / total
        query_step = None
        for index, other in enumerate(visited):
            attention = shifted[index] * inverse
            grad_attention = times(packs[step][3], packs[other][2], 1, 1)
            slope = (attention * (grad_attention - row_dot) * scale_factor).astype(jnp.bfloat16)
            weight_ref[step, index] = attention.astype(jnp.bfloat16)
            slope_ref[step, index] = slope
            part = times(slope, packs[other][1], 1, 0)
            query_step = part if query_step is None else query_step + part
        group, place = groups["q"]
        outs[group * blocks + step][place] = query_step.astype(jnp.bfloat16)
    for step in range(blocks):
        near, far = (step - 1) % blocks, (step - 2) % blocks
        group, place = groups["v"]
        value_step = times(weight_ref[near, 0], packs[near][3], 0, 0) + times(
            weight_ref[far, 1], packs[far][3], 0, 0
        )
        outs[group * blocks + step][place] = value_step.astype(jnp.bfloat16)
        group, place = groups["k"]
        key_step = times(slope_ref[near, 0], packs[near][0], 0, 0) + times(
            slope_ref[far, 1], packs[far][0], 0, 0
        )
        outs[group * blocks + step][place] = key_step.astype(jnp.bfloat16)


def gather_kernel(blocks, count, place_ref, *refs):
    parts = refs[:blocks]
    earlier = refs[blocks : blocks + count]
    keep_ref, send_ref = refs[blocks + count :]
    block, core = place_ref[0], place_ref[1]
    head_size = parts[0].shape[2]
    width = keep_ref.shape[3]
    for step in range(blocks):
        head = lax.rem(block - step + blocks, blocks)
        for which in range(count):
            columns = pl.ds(pl.multiple_of(head * head_size, head_size), head_size)
            total = earlier[which][:, columns] + parts[step][which].astype(jnp.float32)
            for pair in range(head_size // (2 * width)):
                first = total[:, 2 * pair * width : (2 * pair + 1) * width]
                second = total[:, (2 * pair + 1) * width : (2 * pair + 2) * width]
                spot = head * (head_size // (2 * width)) + pair
                keep_ref[which, spot] = jnp.where(core == 0, first, second).astype(jnp.bfloat16)
                send_ref[which, spot] = jnp.where(core == 0, second, first).astype(jnp.bfloat16)


def head_body(
    layer_input,
    queries,
    key_rows,
    value_rows,
    context,
    grad_context,
    grad_output,
    earlier_mass,
    grad_queries,
    grad_keys,
    grad_values,
    documents,
    weights,
    row_factor,
    column_factor,
):
    blocks = lax.axis_size("blk")
    data_count = lax.axis_size("dp")
    block = lax.axis_index("blk")
    data = lax.axis_index("dp")
    core = data % 2
    rows = queries.shape[1]
    units = queries.shape[2]
    features = layer_input.shape[2]
    head_size = units // blocks
    width = units // data_count
    chips = data_count // 2
    in_order = [("v",), ("k",), ("q",)]
    groups = {name: (g, i) for g, names in enumerate(in_order) for i, name in enumerate(names)}
    vmem = pl.BlockSpec(memory_space=pltpu.VMEM)
    smem = pl.BlockSpec(memory_space=pltpu.SMEM)

    def pack(head):
        return jnp.stack(
            [
                lax.dynamic_slice(a[0], (0, head * head_size), (rows, head_size))
                for a in (queries, key_rows, value_rows, grad_context)
            ]
        )

    row_dot = jnp.sum(
        (context[0].astype(jnp.float32) * grad_context[0].astype(jnp.float32)).reshape(
            rows, blocks, head_size
        ),
        axis=2,
    ).T
    doc_rows = jnp.broadcast_to(documents[0].astype(jnp.float32)[None], (blocks, rows))
    side = jnp.stack([earlier_mass[0], row_dot, doc_rows], axis=1)
    side = jnp.pad(side, ((0, 0), (0, 5), (0, 0)))
    packs = [None] * blocks
    sides = [None] * blocks
    packs[0] = pack(block)
    sides[0] = lax.dynamic_index_in_dim(side, block, 0, False)
    for step in range(1, blocks):
        target = (block + step) % blocks
        packs[blocks - step] = rotated(pack(target), step)
        sides[blocks - step] = rotated(lax.dynamic_index_in_dim(side, target, 0, False), step)

    own_input = layer_input[0]
    if data_count == 8:
        mid = rows // 2
        beside, below = swapped(own_input, 2), swapped(own_input, 4)
        across = jnp.concatenate([swapped(beside[:mid], 4), swapped(below[mid:], 2)], axis=0)
        same_core = [own_input, beside, below, across]
    else:
        same_core = [own_input] + [swapped(own_input, m) for m in range(2, data_count, 2)]
    other_core = [swapped(piece, 1) for piece in same_core]
    all_input = jnp.concatenate([p for pair in zip(same_core, other_core) for p in pair], axis=0)

    part_output = jnp.einsum(
        "th,td->dh", context[0], grad_output[0], preferred_element_type=jnp.float32
    ).astype(jnp.bfloat16)

    def columns_for(core_index):
        return jnp.stack(
            [
                lax.dynamic_slice(part_output, (0, (2 * g + core_index) * width), (features, width))
                for g in range(chips)
            ]
        )

    chip_output = (
        columns_for(core).astype(jnp.float32)
        + swapped(columns_for(1 - core), 1).astype(jnp.float32)
    ).astype(jnp.bfloat16)
    output_sum = lax.dynamic_index_in_dim(chip_output, data // 2, 0, False).astype(jnp.float32)
    for m in range(2, data_count, 2):
        output_sum = output_sum + swapped(
            lax.dynamic_index_in_dim(chip_output, (data // 2) ^ (m // 2), 0, False), m
        ).astype(jnp.float32)
    output_part = output_sum.astype(jnp.bfloat16)

    def over_blocks(part):
        pieces = part.reshape(blocks, features // blocks, part.shape[1])
        total = lax.dynamic_index_in_dim(pieces, block, 0, False).astype(jnp.float32)
        for step in range(1, blocks):
            piece = lax.dynamic_index_in_dim(pieces, (block + step) % blocks, 0, False)
            total = total + rotated(piece, step).astype(jnp.float32)
        return total

    shapes = [
        jax.ShapeDtypeStruct((len(names), rows, head_size), jnp.bfloat16)
        for names in in_order
        for step in range(blocks)
    ]
    steps = pl.pallas_call(
        lambda *refs: head_kernel(blocks, groups, *refs),
        out_shape=shapes,
        in_specs=[smem] + [vmem] * (2 * blocks),
        out_specs=[vmem] * len(shapes),
        scratch_shapes=[pltpu.VMEM((blocks, 2, rows, rows), jnp.bfloat16)] * 2,
        name="head_attention",
    )(block.reshape(1), *packs, *sides)
    earlier = {"q": grad_queries[0], "k": grad_keys[0], "v": grad_values[0]}
    place = jnp.stack([block, core])
    partials = {}
    for g, names in enumerate(in_order):
        made = steps[g * blocks : (g + 1) * blocks]
        parts = [made[0]] + [rotated(made[step], step) for step in range(1, blocks)]
        half_shape = jax.ShapeDtypeStruct((len(names), chips, rows, width), jnp.bfloat16)
        keep, send = pl.pallas_call(
            lambda *refs, count=len(names): gather_kernel(blocks, count, *refs),
            out_shape=[half_shape, half_shape],
            in_specs=[smem] + [vmem] * (blocks + len(names)),
            out_specs=[vmem, vmem],
            name="gather_" + "".join(names),
        )(place, *parts, *[earlier[name] for name in names])
        both = jnp.stack([keep, swapped(send, 1)])
        pieces = []
        for m in range(0, data_count, 2):
            piece = lax.dynamic_index_in_dim(both, (data // 2) ^ (m // 2), 2, False)
            pieces.append(swapped(piece, m) if m else piece)
        right = jnp.stack(pieces).transpose(2, 0, 1, 3, 4).reshape(len(names), -1, width)
        for i, name in enumerate(names):
            partials[name] = jnp.einsum(
                "td,tw->dw", all_input, right[i], preferred_element_type=jnp.float32
            ).astype(jnp.bfloat16)
    total_output = over_blocks(output_part)
    summed = {name: over_blocks(partials[name]) for names in in_order for name in names}
    all_tokens = data_count * blocks * rows
    gradient = jnp.stack([summed["q"], summed["k"], summed["v"], total_output]) / all_tokens
    return factored_update(gradient, weights, row_factor, column_factor, blocks, data_count)


def factored_update(gradient, weights, row_factor, column_factor, blocks, data_count):
    full_rows = gradient.shape[1] * blocks
    full_cols = gradient.shape[2] * data_count
    squares = gradient * gradient + tiny_square
    row_sum = lax.psum(jnp.sum(squares, axis=2), "dp")
    new_row_factor = beta_two * row_factor + (1.0 - beta_two) * row_sum / full_cols
    col_sum, row_total = lax.psum(
        (jnp.sum(squares, axis=1), jnp.sum(new_row_factor, axis=1)), "blk"
    )
    new_column_factor = beta_two * column_factor + (1.0 - beta_two) * col_sum / full_rows
    row_mean = row_total / full_rows
    second = new_row_factor[:, :, None] * new_column_factor[:, None, :] / row_mean[:, None, None]
    new_weights = weights - learn_rate * gradient * lax.rsqrt(second)
    return (new_weights, new_row_factor, new_column_factor)


def chosen_body(*arrays):
    blocks = lax.axis_size("blk")
    data_count = lax.axis_size("dp")
    heads = arrays[7].shape[1]
    units = arrays[1].shape[2]
    paired = data_count >= 4 and data_count & (data_count - 1) == 0
    wide = units % (128 * data_count) == 0 and (units // heads) % (2 * units // data_count) == 0
    if heads == blocks and blocks > 2 and paired and wide:
        return head_body(*arrays)
    return ring_body(*arrays)


def solution(mesh):
    placed = (
        P("dp", "blk", None),
        P("dp", "blk", None),
        P("dp", "blk", None),
        P("dp", "blk", None),
        P("dp", "blk", None),
        P("dp", "blk", None),
        P("dp", "blk", None),
        P("dp", None, "blk"),
        P("dp", "blk", None),
        P("dp", "blk", None),
        P("dp", "blk", None),
        P("dp", "blk"),
        P(None, "blk", "dp"),
        P(None, "blk"),
        P(None, "dp"),
    )
    return jax.shard_map(
        chosen_body,
        mesh=mesh,
        in_specs=placed,
        out_specs=(P(None, "blk", "dp"), P(None, "blk"), P(None, "dp")),
        check_vma=False,
    )
```

```python
import math

import jax
import jax.numpy as jnp
from jax import lax
from jax.experimental import pallas as pl
from jax.experimental.pallas import tpu as pltpu
from jax.sharding import PartitionSpec as P


beta_two = 0.9
learn_rate = 0.05
tiny_square = 1e-30


def passed_along(value, axis, steps):
    count = lax.axis_size(axis)
    pairs = [(source, (source + steps) % count) for source in range(count)]
    return lax.ppermute(value, axis, pairs)


def as_sent(array):
    return jax.tree.map(lambda a: a.astype(jnp.bfloat16) if a.dtype == jnp.float32 else a, array)


def folded_rows(block_index, blocks, row_count):
    half = row_count // 2
    local = jnp.arange(row_count, dtype=jnp.int32)
    lower = block_index * half + local
    upper = (2 * blocks - 1 - block_index) * half + local - half
    return jnp.where(local < half, lower, upper)


def attend_back(queries, key_rows, value_rows, context, grad_context, earlier_mass, allowed):
    row_count = queries.shape[0]
    key_count = key_rows.shape[0]
    head_count = earlier_mass.shape[0]
    head_size = queries.shape[1] // head_count
    scale_factor = 1.0 / math.sqrt(head_size)
    query_heads = queries.reshape(row_count, head_count, head_size)
    key_heads = key_rows.reshape(key_count, head_count, head_size)
    value_heads = value_rows.reshape(key_count, head_count, head_size)
    context_heads = context.reshape(row_count, head_count, head_size)
    grad_heads = grad_context.reshape(row_count, head_count, head_size)
    scores = (
        jnp.einsum("thd,shd->hts", query_heads, key_heads, preferred_element_type=jnp.float32)
        * scale_factor
    )
    open_pairs = allowed[None]
    peak_score = jnp.maximum(earlier_mass, jnp.max(jnp.where(open_pairs, scores, -jnp.inf), axis=2))
    shifted = jnp.where(open_pairs, jnp.exp(scores - peak_score[:, :, None]), 0.0)
    total_mass = jnp.exp(earlier_mass - peak_score) + jnp.sum(shifted, axis=2)
    log_norm = peak_score + jnp.log(total_mass)
    attention = jnp.where(open_pairs, jnp.exp(scores - log_norm[:, :, None]), 0.0)
    attention_low = attention.astype(jnp.bfloat16)
    row_dot = jnp.sum(context_heads.astype(jnp.float32) * grad_heads.astype(jnp.float32), axis=2).T
    grad_attention = jnp.einsum(
        "thd,shd->hts", grad_heads, value_heads, preferred_element_type=jnp.float32
    )
    grad_scores = (attention * (grad_attention - row_dot[:, :, None]) * scale_factor).astype(
        jnp.bfloat16
    )
    query_step = jnp.einsum(
        "hts,shd->thd", grad_scores, key_heads, preferred_element_type=jnp.float32
    ).reshape(row_count, -1)
    key_step = jnp.einsum(
        "hts,thd->shd", grad_scores, query_heads, preferred_element_type=jnp.float32
    ).reshape(key_count, -1)
    value_step = jnp.einsum(
        "hts,thd->shd", attention_low, grad_heads, preferred_element_type=jnp.float32
    ).reshape(key_count, -1)
    return (query_step, key_step, value_step)


def ring_body(
    layer_input,
    queries,
    key_rows,
    value_rows,
    context,
    grad_context,
    grad_output,
    earlier_mass,
    grad_queries,
    grad_keys,
    grad_values,
    documents,
    weights,
    row_factor,
    column_factor,
):
    blocks = lax.axis_size("blk")
    data_count = lax.axis_size("dp")
    block_index = lax.axis_index("blk")
    row_count = queries.shape[1]
    own_docs = documents[0]
    doc_float = own_docs.astype(jnp.bfloat16)

    def fetch_next(held):
        return passed_along((held[0], held[1], held[2]), "blk", -1)

    nearer = fetch_next((key_rows[0], value_rows[0], doc_float))
    further = fetch_next(nearer)
    seen_keys = jnp.concatenate([nearer[0], further[0]], axis=0)
    seen_values = jnp.concatenate([nearer[1], further[1]], axis=0)
    seen_docs = jnp.concatenate([nearer[2], further[2]], axis=0).astype(jnp.int32)
    own_pos = folded_rows(block_index, blocks, row_count)
    near_pos = folded_rows((block_index + 1) % blocks, blocks, row_count)
    far_pos = folded_rows((block_index + 2) % blocks, blocks, row_count)
    seen_pos = jnp.concatenate([near_pos, far_pos], axis=0)
    allowed = (seen_pos[None, :] <= own_pos[:, None]) & (seen_docs[None, :] == own_docs[:, None])
    query_step, key_step, value_step = attend_back(
        queries[0], seen_keys, seen_values, context[0], grad_context[0], earlier_mass[0], allowed
    )
    near_part = (key_step[:row_count], value_step[:row_count])
    far_part = (key_step[row_count:], value_step[row_count:])

    def send_back(pair):
        return passed_along((as_sent(pair[0]), as_sent(pair[1])), "blk", 1)

    moved = send_back(far_part)
    home = send_back((moved[0] + near_part[0], moved[1] + near_part[1]))
    query_total = grad_queries[0] + query_step
    key_total = grad_keys[0] + home[0]
    value_total = grad_values[0] + home[1]
    right_low = jnp.stack([query_total, key_total, value_total], axis=1).astype(jnp.bfloat16)
    layer_rows = layer_input[0]
    output_rows = grad_output[0]
    context_rows = context[0]
    all_tokens = data_count * blocks * row_count
    part_inner = jnp.einsum(
        "twh,td->hwd", right_low, layer_rows, preferred_element_type=jnp.float32
    )
    part_output = jnp.einsum(
        "th,td->hd", context_rows, output_rows, preferred_element_type=jnp.float32
    )
    summed = lax.psum_scatter(
        jnp.concatenate([part_inner, part_output[:, None, :]], axis=1).astype(jnp.bfloat16),
        "dp",
        scatter_dimension=0,
        tiled=True,
    )
    grouped = lax.psum_scatter(summed, "blk", scatter_dimension=2, tiled=True).astype(jnp.float32)
    gradient = jnp.transpose(grouped, (1, 2, 0)) / all_tokens
    local_rows = gradient.shape[1]
    local_cols = gradient.shape[2]
    full_rows = local_rows * blocks
    full_cols = local_cols * data_count
    squares = gradient * gradient + tiny_square
    row_part = jnp.sum(squares, axis=2)
    col_part = jnp.sum(squares, axis=1)
    row_sum = lax.psum(row_part, "dp")
    col_sum = lax.psum(col_part, "blk")
    new_row_factor = beta_two * row_factor + (1.0 - beta_two) * row_sum / full_cols
    new_column_factor = beta_two * column_factor + (1.0 - beta_two) * col_sum / full_rows
    row_mean = lax.psum(jnp.sum(new_row_factor, axis=1), "blk") / full_rows
    second = new_row_factor[:, :, None] * new_column_factor[:, None, :] / row_mean[:, None, None]
    new_weights = weights - learn_rate * gradient * lax.rsqrt(second)
    return (new_weights, new_row_factor, new_column_factor)


def swapped(value, mask):
    count = lax.axis_size("dp")
    return lax.ppermute(value, "dp", [(source, source ^ mask) for source in range(count)])


def rotated(value, steps):
    count = lax.axis_size("blk")
    pairs = [(source, (source + steps) % count) for source in range(count)]
    return lax.ppermute(value, "blk", pairs)


def split_three(value):
    high = value.astype(jnp.bfloat16).astype(jnp.float32)
    middle = (value - high).astype(jnp.bfloat16).astype(jnp.float32)
    return (high, middle, value - high - middle)


def pack_kernel(blocks, place_ref, *refs):
    stored, outs = refs[:7], refs[7 : 7 + blocks]
    held, dot_ref, arrived = refs[7 + blocks : 14 + blocks], refs[14 + blocks], refs[15 + blocks]
    copies = [
        pltpu.make_async_copy(source, target, arrived.at[index])
        for index, (source, target) in enumerate(zip(stored, held))
    ]
    for copy in copies:
        copy.start()
    for copy in copies:
        copy.wait()
    query_ref, key_ref, value_ref, grad_ref, context_ref, mass_ref, docs_ref = held
    rows = query_ref.shape[1]
    head_size = query_ref.shape[2] // blocks
    lane = lax.broadcasted_iota(jnp.int32, (rows, 128), 1)
    dots = jnp.zeros((rows, 128), jnp.float32)
    for head in range(blocks):
        columns = slice(head * head_size, (head + 1) * head_size)
        product = context_ref[0, :, columns].astype(jnp.float32) * grad_ref[0, :, columns].astype(
            jnp.float32
        )
        dots = jnp.where(lane == head, jnp.sum(product, axis=1, keepdims=True), dots)
    dot_ref[...] = dots.T
    docs = docs_ref[...].astype(jnp.float32)
    line = lax.broadcasted_iota(jnp.int32, (16, rows), 0)
    for step in range(blocks):
        head = lax.rem(place_ref[0] + step, blocks)
        columns = pl.ds(pl.multiple_of(head * head_size, head_size), head_size)
        for index, ref in enumerate((query_ref, key_ref, value_ref, grad_ref)):
            outs[step][index * rows : (index + 1) * rows] = ref[0, :, columns]
        terms = split_three(mass_ref[0, pl.ds(head, 1), :]) + split_three(dot_ref[pl.ds(head, 1), :])
        side = jnp.where(line == 6, docs, 0.0)
        for index, term in enumerate(terms):
            side = jnp.where(line == index, term, side)
        outs[step][4 * rows :] = side.astype(jnp.bfloat16)


def head_kernel(blocks, place_ref, *refs):
    packs = refs[:blocks]
    value_outs, key_outs, query_outs = (
        refs[(1 + index) * blocks : (2 + index) * blocks] for index in range(3)
    )
    weight_ref, slope_ref = refs[4 * blocks :]
    rows = weight_ref.shape[2]
    half = rows // 2
    scale_factor = 1.0 / math.sqrt(packs[0].shape[1])
    local_down = lax.broadcasted_iota(jnp.int32, (rows, 1), 0)
    local_across = lax.broadcasted_iota(jnp.int32, (1, rows), 1)
    block_of = [lax.rem(place_ref[0] + step, blocks) for step in range(blocks)]

    def part_of(step, index):
        return packs[step][index * rows : (index + 1) * rows]

    def positions(local, block):
        lower = block * half + local
        upper = (2 * blocks - 1 - block) * half + local - half
        return jnp.where(local < half, lower, upper)

    def times(left, right, left_dim, right_dim):
        return lax.dot_general(
            left,
            right,
            (((left_dim,), (right_dim,)), ((), ())),
            preferred_element_type=jnp.float32,
        )

    sides = []
    for step in range(blocks):
        side = packs[step][4 * rows :].astype(jnp.float32)
        mass = side[0:1] + side[1:2] + side[2:3]
        row_dot = side[3:4] + side[4:5] + side[5:6]
        sides.append((mass, row_dot, side[6:7]))
    for step in range(blocks):
        visited = [(step + 1) % blocks, (step + 2) % blocks]
        line = lax.broadcasted_iota(jnp.int32, (8, rows), 0)
        down = jnp.where(line == 0, sides[step][0], jnp.where(line == 1, sides[step][1], sides[step][2])).T
        mass, row_dot, docs = down[:, 0:1], down[:, 1:2], down[:, 2:3]
        own_pos = positions(local_down, block_of[step])
        scored = []
        for other in visited:
            score = times(part_of(step, 0), part_of(other, 1), 1, 1) * scale_factor
            allowed = (positions(local_across, block_of[other]) <= own_pos) & (
                sides[other][2] == docs
            )
            scored.append(jnp.where(allowed, score, -jnp.inf))
        peak = mass
        for score in scored:
            peak = jnp.maximum(peak, jnp.max(score, axis=1, keepdims=True))
        shifted = [jnp.exp(score - peak) for score in scored]
        total = jnp.exp(mass - peak)
        for part in shifted:
            total = total + jnp.sum(part, axis=1, keepdims=True)
        inverse = 1.0 / total
        query_step = None
        for index, other in enumerate(visited):
            attention = shifted[index] * inverse
            grad_attention = times(part_of(step, 3), part_of(other, 2), 1, 1)
            slope = (attention * (grad_attention - row_dot) * scale_factor).astype(jnp.bfloat16)
            weight_ref[step, index] = attention.astype(jnp.bfloat16)
            slope_ref[step, index] = slope
            part = times(slope, part_of(other, 1), 1, 0)
            query_step = part if query_step is None else query_step + part
        query_outs[step][...] = query_step.astype(jnp.bfloat16)
    for step in range(blocks):
        near, far = (step - 1) % blocks, (step - 2) % blocks
        value_step = times(weight_ref[near, 0], part_of(near, 3), 0, 0) + times(
            weight_ref[far, 1], part_of(far, 3), 0, 0
        )
        value_outs[step][...] = value_step.astype(jnp.bfloat16)
        key_step = times(slope_ref[near, 0], part_of(near, 0), 0, 0) + times(
            slope_ref[far, 1], part_of(far, 0), 0, 0
        )
        key_outs[step][...] = key_step.astype(jnp.bfloat16)


def gather_kernel(blocks, place_ref, *refs):
    parts = refs[:blocks]
    earlier = refs[blocks]
    outs = refs[blocks + 1 :]
    head_size = parts[0].shape[1]
    for index in range(blocks):
        head = lax.bitwise_xor(place_ref[1], index)
        source = lax.rem(place_ref[0] - head + blocks, blocks)
        columns = pl.ds(pl.multiple_of(head * head_size, head_size), head_size)
        for step in range(blocks):

            @pl.when(source == step)
            def add(step=step, index=index, columns=columns):
                total = earlier[0, :, columns] + parts[step][...].astype(jnp.float32)
                outs[index][...] = total.astype(jnp.bfloat16)


def weight_kernel(blocks, place_ref, own_ref, beside_ref, below_ref, upper_ref, lower_ref, *refs):
    rights = refs[:blocks]
    keep_ref, send_ref = refs[blocks:]
    features, width = keep_ref.shape
    chunk = features // blocks
    core = place_ref[2]
    for index in range(blocks):
        where = slice(index * chunk, (index + 1) * chunk)
        if index < blocks // 2:
            across = upper_ref[where]
        else:
            across = lower_ref[(index - blocks // 2) * chunk : (index - blocks // 2 + 1) * chunk]
        total = None
        for left, right in zip((own_ref[where], beside_ref[where], below_ref[where], across), rights):
            part = jnp.dot(left, right[...], preferred_element_type=jnp.float32)
            total = part if total is None else total + part
        first, second = total[:, :width], total[:, width:]
        keep_ref[where] = jnp.where(core == 0, first, second)
        send_ref[where] = jnp.where(core == 0, second, first).astype(jnp.bfloat16)


def share_kernel(blocks, place_ref, keep_ref, other_ref, *outs):
    chunk = keep_ref.shape[0] // blocks
    for step in range(blocks):
        start = lax.rem(place_ref[0] + step, blocks) * chunk
        where = pl.ds(pl.multiple_of(start, chunk), chunk)
        total = keep_ref[where] + other_ref[where].astype(jnp.float32)
        outs[step][...] = total.astype(outs[step].dtype)


def head_body(
    layer_input,
    queries,
    key_rows,
    value_rows,
    context,
    grad_context,
    grad_output,
    earlier_mass,
    grad_queries,
    grad_keys,
    grad_values,
    documents,
    weights,
    row_factor,
    column_factor,
):
    blocks = lax.axis_size("blk")
    data_count = lax.axis_size("dp")
    block = lax.axis_index("blk")
    data = lax.axis_index("dp")
    core = data % 2
    chip = data // 2
    rows = queries.shape[1]
    units = queries.shape[2]
    features = layer_input.shape[2]
    head_size = units // blocks
    width = units // data_count
    vmem = pl.BlockSpec(memory_space=pltpu.VMEM)
    smem = pl.BlockSpec(memory_space=pltpu.SMEM)
    place = jnp.stack([block, chip, core])

    def call(kernel, shapes, *arrays, scratch=(), read=vmem, mib=10):
        return pl.pallas_call(
            kernel,
            out_shape=shapes,
            in_specs=[smem] + [read] * len(arrays),
            out_specs=[vmem] * len(shapes),
            scratch_shapes=list(scratch),
            compiler_params=pltpu.CompilerParams(vmem_limit_bytes=mib * 2**20),
        )(place, *arrays)

    def low(*shape):
        return jax.ShapeDtypeStruct(shape, jnp.bfloat16)

    sent = call(
        lambda *refs: pack_kernel(blocks, *refs),
        [low(4 * rows + 16, head_size)] * blocks,
        queries,
        key_rows,
        value_rows,
        grad_context,
        context,
        earlier_mass,
        documents,
        scratch=[pltpu.VMEM((1, rows, units), jnp.bfloat16)] * 5
        + [
            pltpu.VMEM(earlier_mass.shape, jnp.float32),
            pltpu.VMEM(documents.shape, jnp.int32),
            pltpu.VMEM((128, rows), jnp.float32),
            pltpu.SemaphoreType.DMA((7,)),
        ],
        read=pl.BlockSpec(memory_space=pltpu.HBM),
        mib=58,
    )
    packs = [sent[0]] + [None] * (blocks - 1)
    for step in range(1, blocks):
        packs[blocks - step] = rotated(sent[step], step)

    turned = layer_input[0].T
    mid = features // 2
    beside, below = swapped(turned, 2), swapped(turned, 4)
    upper = swapped(beside[:mid], 4)
    lower = swapped(below[mid:], 2)

    part_output = jnp.einsum(
        "th,td->dh", context[0], grad_output[0], preferred_element_type=jnp.float32
    ).astype(jnp.bfloat16)

    def columns_for(core_index):
        return jnp.stack(
            [
                lax.dynamic_slice(part_output, (0, (2 * g + core_index) * width), (features, width))
                for g in range(blocks)
            ]
        )

    chip_output = (
        columns_for(core).astype(jnp.float32)
        + swapped(columns_for(1 - core), 1).astype(jnp.float32)
    ).astype(jnp.bfloat16)
    output_sum = lax.dynamic_index_in_dim(chip_output, chip, 0, False).astype(jnp.float32)
    for m in range(2, data_count, 2):
        output_sum = output_sum + swapped(
            lax.dynamic_index_in_dim(chip_output, chip ^ (m // 2), 0, False), m
        ).astype(jnp.float32)

    steps = call(
        lambda *refs: head_kernel(blocks, *refs),
        [low(rows, head_size)] * (3 * blocks),
        *packs,
        scratch=[pltpu.VMEM((blocks, 2, rows, rows), jnp.bfloat16)] * 2,
    )
    output_pieces = output_sum.reshape(blocks, features // blocks, width)
    totals = {"o": lax.dynamic_index_in_dim(output_pieces, block, 0, False)}
    for step in range(1, blocks):
        piece = lax.dynamic_index_in_dim(output_pieces, (block + step) % blocks, 0, False)
        piece = rotated(piece.astype(jnp.bfloat16), step)
        totals["o"] = totals["o"] + piece.astype(jnp.float32)
    for g, (name, earlier) in enumerate(
        (("v", grad_values), ("k", grad_keys), ("q", grad_queries))
    ):
        made = steps[g * blocks : (g + 1) * blocks]
        parts = [made[0]] + [rotated(made[step], step) for step in range(1, blocks)]
        rights = call(
            lambda *refs: gather_kernel(blocks, *refs),
            [low(rows, head_size)] * blocks,
            *parts,
            earlier,
        )
        rights = [rights[0]] + [swapped(rights[index], 2 * index) for index in range(1, blocks)]
        keep, send = call(
            lambda *refs: weight_kernel(blocks, *refs),
            [jax.ShapeDtypeStruct((features, width), jnp.float32), low(features, width)],
            turned,
            beside,
            below,
            upper,
            lower,
            *rights,
        )
        other = swapped(send, 1)
        shape = (features // blocks, width)
        shares = call(
            lambda *refs: share_kernel(blocks, *refs),
            [jax.ShapeDtypeStruct(shape, jnp.float32)] + [low(*shape)] * (blocks - 1),
            keep,
            other,
        )
        totals[name] = shares[0]
        for step in range(1, blocks):
            piece = rotated(shares[step], step)
            totals[name] = totals[name] + piece.astype(jnp.float32)
    all_tokens = data_count * blocks * rows
    gradient = jnp.stack([totals[name] for name in "qkvo"]) / all_tokens
    return factored_update(gradient, weights, row_factor, column_factor, blocks, data_count)


def factored_update(gradient, weights, row_factor, column_factor, blocks, data_count):
    matrices = gradient.shape[0]
    full_rows = gradient.shape[1] * blocks
    full_cols = gradient.shape[2] * data_count
    lanes = gradient.shape[2]
    squares = gradient * gradient + tiny_square
    row_part = jnp.sum(squares, axis=2)
    factor_part = jnp.sum(row_factor, axis=1, keepdims=True)
    factor_part = jnp.broadcast_to(factor_part, (matrices, lanes))
    sent = jnp.concatenate([jnp.sum(squares, axis=1), factor_part], axis=1)
    along = sent
    for step in range(1, blocks):
        along = along + rotated(sent, step)
    col_sum, factor_sum = along[:, :lanes], along[:, lanes]
    new_column_factor = beta_two * column_factor + (1.0 - beta_two) * col_sum / full_rows
    both = jnp.broadcast_to(jnp.sum(col_sum, axis=1, keepdims=True), (matrices, lanes))
    both = jnp.concatenate([row_part, both], axis=1)
    chips = both
    for m in range(2, data_count, 2):
        chips = chips + swapped(both, m)
    chips = chips + swapped(chips, 1)
    row_sum, all_sum = chips[:, :-lanes], chips[:, -1]
    new_row_factor = beta_two * row_factor + (1.0 - beta_two) * row_sum / full_cols
    row_mean = (beta_two * factor_sum + (1.0 - beta_two) * all_sum / full_cols) / full_rows
    second = new_row_factor[:, :, None] * new_column_factor[:, None, :] / row_mean[:, None, None]
    new_weights = weights - learn_rate * gradient * lax.rsqrt(second)
    return (new_weights, new_row_factor, new_column_factor)


def chosen_body(*arrays):
    blocks = lax.axis_size("blk")
    data_count = lax.axis_size("dp")
    heads = arrays[7].shape[1]
    rows, units = arrays[1].shape[1:]
    head_size = units // heads
    if heads == blocks == 4 and data_count == 2 * blocks and rows == head_size and rows % 128 == 0:
        return head_body(*arrays)
    return ring_body(*arrays)


def solution(mesh):
    placed = (
        P("dp", "blk", None),
        P("dp", "blk", None),
        P("dp", "blk", None),
        P("dp", "blk", None),
        P("dp", "blk", None),
        P("dp", "blk", None),
        P("dp", "blk", None),
        P("dp", None, "blk"),
        P("dp", "blk", None),
        P("dp", "blk", None),
        P("dp", "blk", None),
        P("dp", "blk"),
        P(None, "blk", "dp"),
        P(None, "blk"),
        P(None, "dp"),
    )
    return jax.shard_map(
        chosen_body,
        mesh=mesh,
        in_specs=placed,
        out_specs=(P(None, "blk", "dp"), P(None, "blk"), P(None, "dp")),
        check_vma=False,
    )
```

```python
import math

import jax
import jax.numpy as jnp
from jax import lax
from jax.experimental import pallas as pl
from jax.experimental.pallas import tpu as pltpu
from jax.sharding import PartitionSpec as P


beta_two = 0.9
learn_rate = 0.05
tiny_square = 1e-30


def passed_along(value, axis, steps):
    count = lax.axis_size(axis)
    pairs = [(source, (source + steps) % count) for source in range(count)]
    return lax.ppermute(value, axis, pairs)


def as_sent(array):
    return jax.tree.map(lambda a: a.astype(jnp.bfloat16) if a.dtype == jnp.float32 else a, array)


def folded_rows(block_index, blocks, row_count):
    half = row_count // 2
    local = jnp.arange(row_count, dtype=jnp.int32)
    lower = block_index * half + local
    upper = (2 * blocks - 1 - block_index) * half + local - half
    return jnp.where(local < half, lower, upper)


def attend_back(queries, key_rows, value_rows, context, grad_context, earlier_mass, allowed):
    row_count = queries.shape[0]
    key_count = key_rows.shape[0]
    head_count = earlier_mass.shape[0]
    head_size = queries.shape[1] // head_count
    scale_factor = 1.0 / math.sqrt(head_size)
    query_heads = queries.reshape(row_count, head_count, head_size)
    key_heads = key_rows.reshape(key_count, head_count, head_size)
    value_heads = value_rows.reshape(key_count, head_count, head_size)
    context_heads = context.reshape(row_count, head_count, head_size)
    grad_heads = grad_context.reshape(row_count, head_count, head_size)
    scores = (
        jnp.einsum("thd,shd->hts", query_heads, key_heads, preferred_element_type=jnp.float32)
        * scale_factor
    )
    open_pairs = allowed[None]
    peak_score = jnp.maximum(earlier_mass, jnp.max(jnp.where(open_pairs, scores, -jnp.inf), axis=2))
    shifted = jnp.where(open_pairs, jnp.exp(scores - peak_score[:, :, None]), 0.0)
    total_mass = jnp.exp(earlier_mass - peak_score) + jnp.sum(shifted, axis=2)
    log_norm = peak_score + jnp.log(total_mass)
    attention = jnp.where(open_pairs, jnp.exp(scores - log_norm[:, :, None]), 0.0)
    attention_low = attention.astype(jnp.bfloat16)
    row_dot = jnp.sum(context_heads.astype(jnp.float32) * grad_heads.astype(jnp.float32), axis=2).T
    grad_attention = jnp.einsum(
        "thd,shd->hts", grad_heads, value_heads, preferred_element_type=jnp.float32
    )
    grad_scores = (attention * (grad_attention - row_dot[:, :, None]) * scale_factor).astype(
        jnp.bfloat16
    )
    query_step = jnp.einsum(
        "hts,shd->thd", grad_scores, key_heads, preferred_element_type=jnp.float32
    ).reshape(row_count, -1)
    key_step = jnp.einsum(
        "hts,thd->shd", grad_scores, query_heads, preferred_element_type=jnp.float32
    ).reshape(key_count, -1)
    value_step = jnp.einsum(
        "hts,thd->shd", attention_low, grad_heads, preferred_element_type=jnp.float32
    ).reshape(key_count, -1)
    return (query_step, key_step, value_step)


def ring_body(
    layer_input,
    queries,
    key_rows,
    value_rows,
    context,
    grad_context,
    grad_output,
    earlier_mass,
    grad_queries,
    grad_keys,
    grad_values,
    documents,
    weights,
    row_factor,
    column_factor,
):
    blocks = lax.axis_size("blk")
    data_count = lax.axis_size("dp")
    block_index = lax.axis_index("blk")
    row_count = queries.shape[1]
    own_docs = documents[0]
    doc_float = own_docs.astype(jnp.bfloat16)

    def fetch_next(held):
        return passed_along((held[0], held[1], held[2]), "blk", -1)

    nearer = fetch_next((key_rows[0], value_rows[0], doc_float))
    further = fetch_next(nearer)
    seen_keys = jnp.concatenate([nearer[0], further[0]], axis=0)
    seen_values = jnp.concatenate([nearer[1], further[1]], axis=0)
    seen_docs = jnp.concatenate([nearer[2], further[2]], axis=0).astype(jnp.int32)
    own_pos = folded_rows(block_index, blocks, row_count)
    near_pos = folded_rows((block_index + 1) % blocks, blocks, row_count)
    far_pos = folded_rows((block_index + 2) % blocks, blocks, row_count)
    seen_pos = jnp.concatenate([near_pos, far_pos], axis=0)
    allowed = (seen_pos[None, :] <= own_pos[:, None]) & (seen_docs[None, :] == own_docs[:, None])
    query_step, key_step, value_step = attend_back(
        queries[0], seen_keys, seen_values, context[0], grad_context[0], earlier_mass[0], allowed
    )
    near_part = (key_step[:row_count], value_step[:row_count])
    far_part = (key_step[row_count:], value_step[row_count:])

    def send_back(pair):
        return passed_along((as_sent(pair[0]), as_sent(pair[1])), "blk", 1)

    moved = send_back(far_part)
    home = send_back((moved[0] + near_part[0], moved[1] + near_part[1]))
    query_total = grad_queries[0] + query_step
    key_total = grad_keys[0] + home[0]
    value_total = grad_values[0] + home[1]
    right_low = jnp.stack([query_total, key_total, value_total], axis=1).astype(jnp.bfloat16)
    layer_rows = layer_input[0]
    output_rows = grad_output[0]
    context_rows = context[0]
    all_tokens = data_count * blocks * row_count
    part_inner = jnp.einsum(
        "twh,td->hwd", right_low, layer_rows, preferred_element_type=jnp.float32
    )
    part_output = jnp.einsum(
        "th,td->hd", context_rows, output_rows, preferred_element_type=jnp.float32
    )
    summed = lax.psum_scatter(
        jnp.concatenate([part_inner, part_output[:, None, :]], axis=1).astype(jnp.bfloat16),
        "dp",
        scatter_dimension=0,
        tiled=True,
    )
    grouped = lax.psum_scatter(summed, "blk", scatter_dimension=2, tiled=True).astype(jnp.float32)
    gradient = jnp.transpose(grouped, (1, 2, 0)) / all_tokens
    local_rows = gradient.shape[1]
    local_cols = gradient.shape[2]
    full_rows = local_rows * blocks
    full_cols = local_cols * data_count
    squares = gradient * gradient + tiny_square
    row_part = jnp.sum(squares, axis=2)
    col_part = jnp.sum(squares, axis=1)
    row_sum = lax.psum(row_part, "dp")
    col_sum = lax.psum(col_part, "blk")
    new_row_factor = beta_two * row_factor + (1.0 - beta_two) * row_sum / full_cols
    new_column_factor = beta_two * column_factor + (1.0 - beta_two) * col_sum / full_rows
    row_mean = lax.psum(jnp.sum(new_row_factor, axis=1), "blk") / full_rows
    second = new_row_factor[:, :, None] * new_column_factor[:, None, :] / row_mean[:, None, None]
    new_weights = weights - learn_rate * gradient * lax.rsqrt(second)
    return (new_weights, new_row_factor, new_column_factor)


def swapped(value, mask):
    count = lax.axis_size("dp")
    return lax.ppermute(value, "dp", [(source, source ^ mask) for source in range(count)])


def rotated(value, steps):
    count = lax.axis_size("blk")
    pairs = [(source, (source + steps) % count) for source in range(count)]
    return lax.ppermute(value, "blk", pairs)


def traded(value, mask):
    count = lax.axis_size("blk")
    return lax.ppermute(value, "blk", [(source, source ^ mask) for source in range(count)])


def split_three(value):
    high = value.astype(jnp.bfloat16).astype(jnp.float32)
    middle = (value - high).astype(jnp.bfloat16).astype(jnp.float32)
    return (high, middle, value - high - middle)


def pack_kernel(blocks, place_ref, *refs):
    stored, outs = refs[:7], refs[7 : 7 + blocks]
    held, dot_ref, arrived = refs[7 + blocks : 14 + blocks], refs[14 + blocks], refs[15 + blocks]
    copies = [
        pltpu.make_async_copy(source, target, arrived.at[index])
        for index, (source, target) in enumerate(zip(stored, held))
    ]
    for copy in copies:
        copy.start()
    for copy in copies:
        copy.wait()
    query_ref, key_ref, value_ref, grad_ref, context_ref, mass_ref, docs_ref = held
    rows = query_ref.shape[1]
    head_size = query_ref.shape[2] // blocks
    lane = lax.broadcasted_iota(jnp.int32, (rows, 128), 1)
    dots = jnp.zeros((rows, 128), jnp.float32)
    for head in range(blocks):
        columns = slice(head * head_size, (head + 1) * head_size)
        product = context_ref[0, :, columns].astype(jnp.float32) * grad_ref[0, :, columns].astype(
            jnp.float32
        )
        dots = jnp.where(lane == head, jnp.sum(product, axis=1, keepdims=True), dots)
    dot_ref[...] = dots.T
    docs = docs_ref[...].astype(jnp.float32)
    line = lax.broadcasted_iota(jnp.int32, (16, rows), 0)
    for step in range(blocks):
        head = lax.rem(place_ref[0] + step, blocks)
        columns = pl.ds(pl.multiple_of(head * head_size, head_size), head_size)
        for index, ref in enumerate((query_ref, key_ref, value_ref, grad_ref)):
            outs[step][index * rows : (index + 1) * rows] = ref[0, :, columns]
        terms = split_three(mass_ref[0, pl.ds(head, 1), :]) + split_three(dot_ref[pl.ds(head, 1), :])
        side = jnp.where(line == 6, docs, 0.0)
        for index, term in enumerate(terms):
            side = jnp.where(line == index, term, side)
        outs[step][4 * rows :] = side.astype(jnp.bfloat16)


def times(left, right, left_dim, right_dim):
    return lax.dot_general(
        left,
        right,
        (((left_dim,), (right_dim,)), ((), ())),
        preferred_element_type=jnp.float32,
    )


def side_of(pack_ref):
    rows = (pack_ref.shape[0] - 16) // 4
    side = pack_ref[4 * rows :].astype(jnp.float32)
    return side[0:1] + side[1:2] + side[2:3], side[3:4] + side[4:5] + side[5:6], side[6:7]


def part_of(pack_ref, index):
    rows = (pack_ref.shape[0] - 16) // 4
    return pack_ref[index * rows : (index + 1) * rows]


def weigh_kernel(blocks, place_ref, *refs):
    packs, outs, weight_ref = refs[:blocks], refs[blocks : 2 * blocks], refs[2 * blocks]
    rows = weight_ref.shape[2]
    half = rows // 2
    scale_factor = 1.0 / math.sqrt(packs[0].shape[1])
    local_down = lax.broadcasted_iota(jnp.int32, (rows, 1), 0)
    local_across = lax.broadcasted_iota(jnp.int32, (1, rows), 1)
    line = lax.broadcasted_iota(jnp.int32, (8, rows), 0)
    block_of = [lax.rem(place_ref[0] + step, blocks) for step in range(blocks)]

    def positions(local, block):
        lower = block * half + local
        upper = (2 * blocks - 1 - block) * half + local - half
        return jnp.where(local < half, lower, upper)

    for step in range(blocks):
        mass, _, docs = side_of(packs[step])
        down = jnp.where(line == 0, mass, docs).T
        mass, docs = down[:, 0:1], down[:, 1:2]
        own_pos = positions(local_down, block_of[step])
        scored = []
        for far in range(2):
            other = (step + 1 + far) % blocks
            score = times(part_of(packs[step], 0), part_of(packs[other], 1), 1, 1) * scale_factor
            allowed = (positions(local_across, block_of[other]) <= own_pos) & (
                side_of(packs[other])[2] == docs
            )
            scored.append(jnp.where(allowed, score, -jnp.inf))
        peak = mass
        for score in scored:
            peak = jnp.maximum(peak, jnp.max(score, axis=1, keepdims=True))
        shifted = [jnp.exp(score - peak) for score in scored]
        total = jnp.exp(mass - peak)
        for part in shifted:
            total = total + jnp.sum(part, axis=1, keepdims=True)
        inverse = 1.0 / total
        for far in range(2):
            weight_ref[step, far] = (shifted[far] * inverse).astype(weight_ref.dtype)
    for step in range(blocks):
        near, far = (step - 1) % blocks, (step - 2) % blocks
        value_step = times(
            weight_ref[near, 0].astype(jnp.bfloat16), part_of(packs[near], 3), 0, 0
        ) + times(weight_ref[far, 1].astype(jnp.bfloat16), part_of(packs[far], 3), 0, 0)
        outs[step][...] = value_step.astype(jnp.bfloat16)


def slope_kernel(blocks, place_ref, weight_ref, *refs):
    packs, key_outs, query_outs = (refs[n * blocks : (n + 1) * blocks] for n in range(3))
    slope_ref = refs[3 * blocks]
    rows = weight_ref.shape[2]
    scale_factor = 1.0 / math.sqrt(packs[0].shape[1])
    line = lax.broadcasted_iota(jnp.int32, (8, rows), 0)
    for step in range(blocks):
        row_dot = jnp.where(line == 0, side_of(packs[step])[1], 0.0).T[:, 0:1]
        query_step = None
        for far in range(2):
            other = (step + 1 + far) % blocks
            grad_attention = times(part_of(packs[step], 3), part_of(packs[other], 2), 1, 1)
            slope = weight_ref[step, far] * (grad_attention - row_dot) * scale_factor
            slope = slope.astype(jnp.bfloat16)
            slope_ref[step, far] = slope
            part = times(slope, part_of(packs[other], 1), 1, 0)
            query_step = part if query_step is None else query_step + part
        query_outs[step][...] = query_step.astype(jnp.bfloat16)
    for step in range(blocks):
        near, far = (step - 1) % blocks, (step - 2) % blocks
        key_step = times(slope_ref[near, 0], part_of(packs[near], 0), 0, 0) + times(
            slope_ref[far, 1], part_of(packs[far], 0), 0, 0
        )
        key_outs[step][...] = key_step.astype(jnp.bfloat16)


def gather_kernel(blocks, place_ref, *refs):
    parts = refs[:blocks]
    earlier = refs[blocks]
    outs = refs[blocks + 1 :]
    head_size = parts[0].shape[1]
    for index in range(blocks):
        head = lax.bitwise_xor(place_ref[1], index)
        source = lax.rem(place_ref[0] - head + blocks, blocks)
        columns = pl.ds(pl.multiple_of(head * head_size, head_size), head_size)
        for step in range(blocks):

            @pl.when(source == step)
            def add(step=step, index=index, columns=columns):
                total = earlier[0, :, columns] + parts[step][...].astype(jnp.float32)
                outs[index][...] = total.astype(jnp.bfloat16)


def weight_kernel(blocks, place_ref, own_ref, beside_ref, below_ref, upper_ref, lower_ref, *refs):
    rights = refs[:blocks]
    keep_ref, send_ref = refs[blocks:]
    features, width = keep_ref.shape
    chunk = features // blocks
    core = place_ref[2]
    for index in range(blocks):
        where = slice(index * chunk, (index + 1) * chunk)
        if index < blocks // 2:
            across = upper_ref[where]
        else:
            across = lower_ref[(index - blocks // 2) * chunk : (index - blocks // 2 + 1) * chunk]
        total = None
        for left, right in zip((own_ref[where], beside_ref[where], below_ref[where], across), rights):
            part = jnp.dot(left, right[...], preferred_element_type=jnp.float32)
            total = part if total is None else total + part
        first, second = total[:, :width], total[:, width:]
        keep_ref[where] = jnp.where(core == 0, first, second).astype(jnp.bfloat16)
        send_ref[where] = jnp.where(core == 0, second, first).astype(jnp.bfloat16)


def near_kernel(place_ref, *refs):
    parts = refs[:-2]
    keep_ref, send_ref = refs[-2:]
    chunk = keep_ref.shape[1]
    side = lax.bitwise_and(place_ref[0], 1)
    for index in range(2):
        for ref, parity in ((keep_ref, side), (send_ref, 1 - side)):
            where = pl.ds(pl.multiple_of((2 * index + parity) * chunk, chunk), chunk)
            total = parts[0][where].astype(jnp.float32)
            for part in parts[1:]:
                total = total + part[where].astype(jnp.float32)
            ref[index] = total.astype(ref.dtype)


def far_kernel(place_ref, held_ref, other_ref, keep_ref, send_ref):
    side = lax.div(place_ref[0], 2)
    keep_ref[...] = held_ref[side] + other_ref[side].astype(jnp.float32)
    total = held_ref[1 - side] + other_ref[1 - side].astype(jnp.float32)
    send_ref[...] = total.astype(jnp.bfloat16)


def head_body(
    layer_input,
    queries,
    key_rows,
    value_rows,
    context,
    grad_context,
    grad_output,
    earlier_mass,
    grad_queries,
    grad_keys,
    grad_values,
    documents,
    weights,
    row_factor,
    column_factor,
):
    blocks = lax.axis_size("blk")
    data_count = lax.axis_size("dp")
    block = lax.axis_index("blk")
    data = lax.axis_index("dp")
    core = data % 2
    chip = data // 2
    rows = queries.shape[1]
    units = queries.shape[2]
    features = layer_input.shape[2]
    head_size = units // blocks
    width = units // data_count
    vmem = pl.BlockSpec(memory_space=pltpu.VMEM)
    smem = pl.BlockSpec(memory_space=pltpu.SMEM)
    place = jnp.stack([block, chip, core])

    def call(kernel, shapes, *arrays, scratch=(), read=vmem, mib=4):
        return pl.pallas_call(
            kernel,
            out_shape=shapes,
            in_specs=[smem] + [read] * len(arrays),
            out_specs=[vmem] * len(shapes),
            scratch_shapes=list(scratch),
            compiler_params=pltpu.CompilerParams(vmem_limit_bytes=mib * 2**20),
        )(place, *arrays)

    def low(*shape):
        return jax.ShapeDtypeStruct(shape, jnp.bfloat16)

    sent = call(
        lambda *refs: pack_kernel(blocks, *refs),
        [low(4 * rows + 16, head_size)] * blocks,
        queries,
        key_rows,
        value_rows,
        grad_context,
        context,
        earlier_mass,
        documents,
        scratch=[pltpu.VMEM((1, rows, units), jnp.bfloat16)] * 5
        + [
            pltpu.VMEM(earlier_mass.shape, jnp.float32),
            pltpu.VMEM(documents.shape, jnp.int32),
            pltpu.VMEM((128, rows), jnp.float32),
            pltpu.SemaphoreType.DMA((7,)),
        ],
        read=pl.BlockSpec(memory_space=pltpu.HBM),
        mib=58,
    )
    packs = [sent[0]] + [None] * (blocks - 1)
    for step in range(1, blocks):
        packs[blocks - step] = rotated(sent[step], step)

    turned = layer_input[0].T
    mid = features // 2
    beside, below = swapped(turned, 2), swapped(turned, 4)
    upper = swapped(beside[:mid], 4)
    lower = swapped(below[mid:], 2)

    part_output = jnp.einsum(
        "th,td->dh", context[0], grad_output[0], preferred_element_type=jnp.float32
    ).astype(jnp.bfloat16)

    def columns_for(core_index):
        return jnp.stack(
            [
                lax.dynamic_slice(part_output, (0, (2 * g + core_index) * width), (features, width))
                for g in range(blocks)
            ]
        )

    chip_output = (
        columns_for(core).astype(jnp.float32)
        + swapped(columns_for(1 - core), 1).astype(jnp.float32)
    ).astype(jnp.bfloat16)
    output_parts = [lax.dynamic_index_in_dim(chip_output, chip, 0, False)]
    for m in range(2, data_count, 2):
        piece = lax.dynamic_index_in_dim(chip_output, chip ^ (m // 2), 0, False)
        output_parts.append(swapped(piece, m))

    def halved(*parts):
        chunk = features // blocks
        wide = jax.ShapeDtypeStruct((2, chunk, width), jnp.float32)
        held, sent = call(near_kernel, [wide, low(2, chunk, width)], *parts)
        other = traded(sent, 1)
        narrow = jax.ShapeDtypeStruct((chunk, width), jnp.float32)
        held, sent = call(far_kernel, [narrow, low(chunk, width)], held, other)
        return held, traded(sent, 2)

    weighed = call(
        lambda *refs: weigh_kernel(blocks, *refs),
        [low(rows, head_size)] * blocks
        + [jax.ShapeDtypeStruct((blocks, 2, rows, rows), jnp.float32)],
        *packs,
        mib=12,
    )
    sloped = call(
        lambda *refs: slope_kernel(blocks, *refs),
        [low(rows, head_size)] * (2 * blocks),
        weighed[blocks],
        *packs,
        scratch=[pltpu.VMEM((blocks, 2, rows, rows), jnp.bfloat16)],
        mib=12,
    )
    steps = list(weighed[:blocks]) + list(sloped)
    totals = {"o": halved(*output_parts)}
    for g, (name, earlier) in enumerate(
        (("v", grad_values), ("k", grad_keys), ("q", grad_queries))
    ):
        made = steps[g * blocks : (g + 1) * blocks]
        parts = [made[0]] + [rotated(made[step], step) for step in range(1, blocks)]
        rights = call(
            lambda *refs: gather_kernel(blocks, *refs),
            [low(rows, head_size)] * blocks,
            *parts,
            earlier,
        )
        rights = [rights[0]] + [swapped(rights[index], 2 * index) for index in range(1, blocks)]
        keep, send = call(
            lambda *refs: weight_kernel(blocks, *refs),
            [low(features, width)] * 2,
            turned,
            beside,
            below,
            upper,
            lower,
            *rights,
        )
        other = swapped(send, 1)
        totals[name] = halved(keep, other)
    totals = {
        name: sum(part.astype(jnp.float32) for part in parts) for name, parts in totals.items()
    }
    all_tokens = data_count * blocks * rows
    gradient = jnp.stack([totals[name] for name in "qkvo"]) / all_tokens
    return factored_update(gradient, weights, row_factor, column_factor, blocks, data_count)


def factored_update(gradient, weights, row_factor, column_factor, blocks, data_count):
    matrices = gradient.shape[0]
    full_rows = gradient.shape[1] * blocks
    full_cols = gradient.shape[2] * data_count
    lanes = gradient.shape[2]
    squares = gradient * gradient + tiny_square
    row_part = jnp.sum(squares, axis=2)
    factor_part = jnp.sum(row_factor, axis=1, keepdims=True)
    factor_part = jnp.broadcast_to(factor_part, (matrices, lanes))
    sent = jnp.concatenate([jnp.sum(squares, axis=1), factor_part], axis=1)
    along = sent
    for step in range(1, blocks):
        along = along + rotated(sent, step)
    col_sum, factor_sum = along[:, :lanes], along[:, lanes]
    new_column_factor = beta_two * column_factor + (1.0 - beta_two) * col_sum / full_rows
    both = jnp.broadcast_to(jnp.sum(col_sum, axis=1, keepdims=True), (matrices, lanes))
    both = jnp.concatenate([row_part, both], axis=1)
    chips = both
    for m in range(2, data_count, 2):
        chips = chips + swapped(both, m)
    chips = chips + swapped(chips, 1)
    row_sum, all_sum = chips[:, :-lanes], chips[:, -1]
    new_row_factor = beta_two * row_factor + (1.0 - beta_two) * row_sum / full_cols
    row_mean = (beta_two * factor_sum + (1.0 - beta_two) * all_sum / full_cols) / full_rows
    second = new_row_factor[:, :, None] * new_column_factor[:, None, :] / row_mean[:, None, None]
    new_weights = weights - learn_rate * gradient * lax.rsqrt(second)
    return (new_weights, new_row_factor, new_column_factor)


def chosen_body(*arrays):
    blocks = lax.axis_size("blk")
    data_count = lax.axis_size("dp")
    heads = arrays[7].shape[1]
    rows, units = arrays[1].shape[1:]
    head_size = units // heads
    if heads == blocks == 4 and data_count == 2 * blocks and rows == head_size and rows % 128 == 0:
        return head_body(*arrays)
    return ring_body(*arrays)


def solution(mesh):
    placed = (
        P("dp", "blk", None),
        P("dp", "blk", None),
        P("dp", "blk", None),
        P("dp", "blk", None),
        P("dp", "blk", None),
        P("dp", "blk", None),
        P("dp", "blk", None),
        P("dp", None, "blk"),
        P("dp", "blk", None),
        P("dp", "blk", None),
        P("dp", "blk", None),
        P("dp", "blk"),
        P(None, "blk", "dp"),
        P(None, "blk"),
        P(None, "dp"),
    )
    return jax.shard_map(
        chosen_body,
        mesh=mesh,
        in_specs=placed,
        out_specs=(P(None, "blk", "dp"), P(None, "blk"), P(None, "dp")),
        check_vma=False,
    )
```

```python
import math

import jax
import jax.numpy as jnp
from jax import lax
from jax.experimental import pallas as pl
from jax.experimental.pallas import tpu as pltpu
from jax.sharding import PartitionSpec as P


beta_two = 0.9
learn_rate = 0.05
tiny_square = 1e-30


def passed_along(value, axis, steps):
    count = lax.axis_size(axis)
    pairs = [(source, (source + steps) % count) for source in range(count)]
    return lax.ppermute(value, axis, pairs)


def as_sent(array):
    return jax.tree.map(lambda a: a.astype(jnp.bfloat16) if a.dtype == jnp.float32 else a, array)


def folded_rows(block_index, blocks, row_count):
    half = row_count // 2
    local = jnp.arange(row_count, dtype=jnp.int32)
    lower = block_index * half + local
    upper = (2 * blocks - 1 - block_index) * half + local - half
    return jnp.where(local < half, lower, upper)


def attend_back(queries, key_rows, value_rows, context, grad_context, earlier_mass, allowed):
    row_count = queries.shape[0]
    key_count = key_rows.shape[0]
    head_count = earlier_mass.shape[0]
    head_size = queries.shape[1] // head_count
    scale_factor = 1.0 / math.sqrt(head_size)
    query_heads = queries.reshape(row_count, head_count, head_size)
    key_heads = key_rows.reshape(key_count, head_count, head_size)
    value_heads = value_rows.reshape(key_count, head_count, head_size)
    context_heads = context.reshape(row_count, head_count, head_size)
    grad_heads = grad_context.reshape(row_count, head_count, head_size)
    scores = (
        jnp.einsum("thd,shd->hts", query_heads, key_heads, preferred_element_type=jnp.float32)
        * scale_factor
    )
    open_pairs = allowed[None]
    peak_score = jnp.maximum(earlier_mass, jnp.max(jnp.where(open_pairs, scores, -jnp.inf), axis=2))
    shifted = jnp.where(open_pairs, jnp.exp(scores - peak_score[:, :, None]), 0.0)
    total_mass = jnp.exp(earlier_mass - peak_score) + jnp.sum(shifted, axis=2)
    log_norm = peak_score + jnp.log(total_mass)
    attention = jnp.where(open_pairs, jnp.exp(scores - log_norm[:, :, None]), 0.0)
    attention_low = attention.astype(jnp.bfloat16)
    row_dot = jnp.sum(context_heads.astype(jnp.float32) * grad_heads.astype(jnp.float32), axis=2).T
    grad_attention = jnp.einsum(
        "thd,shd->hts", grad_heads, value_heads, preferred_element_type=jnp.float32
    )
    grad_scores = (attention * (grad_attention - row_dot[:, :, None]) * scale_factor).astype(
        jnp.bfloat16
    )
    query_step = jnp.einsum(
        "hts,shd->thd", grad_scores, key_heads, preferred_element_type=jnp.float32
    ).reshape(row_count, -1)
    key_step = jnp.einsum(
        "hts,thd->shd", grad_scores, query_heads, preferred_element_type=jnp.float32
    ).reshape(key_count, -1)
    value_step = jnp.einsum(
        "hts,thd->shd", attention_low, grad_heads, preferred_element_type=jnp.float32
    ).reshape(key_count, -1)
    return (query_step, key_step, value_step)


def ring_body(
    layer_input,
    queries,
    key_rows,
    value_rows,
    context,
    grad_context,
    grad_output,
    earlier_mass,
    grad_queries,
    grad_keys,
    grad_values,
    documents,
    weights,
    row_factor,
    column_factor,
):
    blocks = lax.axis_size("blk")
    data_count = lax.axis_size("dp")
    block_index = lax.axis_index("blk")
    row_count = queries.shape[1]
    own_docs = documents[0]
    doc_float = own_docs.astype(jnp.bfloat16)

    def fetch_next(held):
        return passed_along((held[0], held[1], held[2]), "blk", -1)

    nearer = fetch_next((key_rows[0], value_rows[0], doc_float))
    further = fetch_next(nearer)
    seen_keys = jnp.concatenate([nearer[0], further[0]], axis=0)
    seen_values = jnp.concatenate([nearer[1], further[1]], axis=0)
    seen_docs = jnp.concatenate([nearer[2], further[2]], axis=0).astype(jnp.int32)
    own_pos = folded_rows(block_index, blocks, row_count)
    near_pos = folded_rows((block_index + 1) % blocks, blocks, row_count)
    far_pos = folded_rows((block_index + 2) % blocks, blocks, row_count)
    seen_pos = jnp.concatenate([near_pos, far_pos], axis=0)
    allowed = (seen_pos[None, :] <= own_pos[:, None]) & (seen_docs[None, :] == own_docs[:, None])
    query_step, key_step, value_step = attend_back(
        queries[0], seen_keys, seen_values, context[0], grad_context[0], earlier_mass[0], allowed
    )
    near_part = (key_step[:row_count], value_step[:row_count])
    far_part = (key_step[row_count:], value_step[row_count:])

    def send_back(pair):
        return passed_along((as_sent(pair[0]), as_sent(pair[1])), "blk", 1)

    moved = send_back(far_part)
    home = send_back((moved[0] + near_part[0], moved[1] + near_part[1]))
    query_total = grad_queries[0] + query_step
    key_total = grad_keys[0] + home[0]
    value_total = grad_values[0] + home[1]
    right_low = jnp.stack([query_total, key_total, value_total], axis=1).astype(jnp.bfloat16)
    layer_rows = layer_input[0]
    output_rows = grad_output[0]
    context_rows = context[0]
    all_tokens = data_count * blocks * row_count
    part_inner = jnp.einsum(
        "twh,td->hwd", right_low, layer_rows, preferred_element_type=jnp.float32
    )
    part_output = jnp.einsum(
        "th,td->hd", context_rows, output_rows, preferred_element_type=jnp.float32
    )
    summed = lax.psum_scatter(
        jnp.concatenate([part_inner, part_output[:, None, :]], axis=1).astype(jnp.bfloat16),
        "dp",
        scatter_dimension=0,
        tiled=True,
    )
    grouped = lax.psum_scatter(summed, "blk", scatter_dimension=2, tiled=True).astype(jnp.float32)
    gradient = jnp.transpose(grouped, (1, 2, 0)) / all_tokens
    local_rows = gradient.shape[1]
    local_cols = gradient.shape[2]
    full_rows = local_rows * blocks
    full_cols = local_cols * data_count
    squares = gradient * gradient + tiny_square
    row_part = jnp.sum(squares, axis=2)
    col_part = jnp.sum(squares, axis=1)
    row_sum = lax.psum(row_part, "dp")
    col_sum = lax.psum(col_part, "blk")
    new_row_factor = beta_two * row_factor + (1.0 - beta_two) * row_sum / full_cols
    new_column_factor = beta_two * column_factor + (1.0 - beta_two) * col_sum / full_rows
    row_mean = lax.psum(jnp.sum(new_row_factor, axis=1), "blk") / full_rows
    second = new_row_factor[:, :, None] * new_column_factor[:, None, :] / row_mean[:, None, None]
    new_weights = weights - learn_rate * gradient * lax.rsqrt(second)
    return (new_weights, new_row_factor, new_column_factor)


def swapped(value, mask):
    count = lax.axis_size("dp")
    return lax.ppermute(value, "dp", [(source, source ^ mask) for source in range(count)])


def rotated(value, steps):
    count = lax.axis_size("blk")
    pairs = [(source, (source + steps) % count) for source in range(count)]
    return lax.ppermute(value, "blk", pairs)


def traded(value, mask):
    count = lax.axis_size("blk")
    return lax.ppermute(value, "blk", [(source, source ^ mask) for source in range(count)])


def split_three(value):
    high = value.astype(jnp.bfloat16).astype(jnp.float32)
    middle = (value - high).astype(jnp.bfloat16).astype(jnp.float32)
    return (high, middle, value - high - middle)


def pack_heads(blocks, place_ref, stored, outs, arrived):
    rows = stored[0].shape[1]
    head_size = stored[0].shape[2] // blocks
    copies = []
    for step in range(blocks):
        head = lax.rem(place_ref[0] + step, blocks)
        columns = pl.ds(pl.multiple_of(head * head_size, head_size), head_size)
        for index, ref in enumerate(stored):
            target = outs[step].at[index * rows : (index + 1) * rows]
            copies.append(
                pltpu.make_async_copy(ref.at[0, :, columns], target, arrived.at[len(copies)])
            )
    for copy in copies:
        copy.start()
    return copies


def held_copies(stored, held, arrived, first):
    copies = [
        pltpu.make_async_copy(source, target, arrived.at[first + index])
        for index, (source, target) in enumerate(zip(stored, held))
    ]
    for copy in copies:
        copy.start()
    return copies


def pack_early_kernel(blocks, place_ref, query_ref, key_ref, mass_ref, docs_ref, *refs):
    outs, held, arrived = refs[:blocks], refs[blocks : blocks + 2], refs[blocks + 2]
    small = held_copies((mass_ref, docs_ref), held, arrived, 2 * blocks)
    copies = pack_heads(blocks, place_ref, (query_ref, key_ref), outs, arrived)
    rows = docs_ref.shape[1]
    line = lax.broadcasted_iota(jnp.int32, (16, rows), 0)
    for copy in small:
        copy.wait()
    docs = held[1][...].astype(jnp.float32)
    for step in range(blocks):
        head = lax.rem(place_ref[0] + step, blocks)
        side = jnp.where(line == 3, docs, 0.0)
        for index, term in enumerate(split_three(held[0][0, pl.ds(head, 1), :])):
            side = jnp.where(line == index, term, side)
        outs[step][2 * rows :] = side.astype(jnp.bfloat16)
    for copy in copies:
        copy.wait()


def pack_late_kernel(blocks, place_ref, value_ref, grad_ref, context_ref, *refs):
    outs, held = refs[:blocks], refs[blocks : blocks + 2]
    dot_ref, arrived = refs[blocks + 2 :]
    large = held_copies((grad_ref, context_ref), held, arrived, 2 * blocks)
    copies = pack_heads(blocks, place_ref, (value_ref, grad_ref), outs, arrived)
    rows = value_ref.shape[1]
    head_size = value_ref.shape[2] // blocks
    for copy in large:
        copy.wait()
    lane = lax.broadcasted_iota(jnp.int32, (rows, 128), 1)
    dots = jnp.zeros((rows, 128), jnp.float32)
    for head in range(blocks):
        columns = slice(head * head_size, (head + 1) * head_size)
        product = held[0][0, :, columns].astype(jnp.float32) * held[1][0, :, columns].astype(
            jnp.float32
        )
        dots = jnp.where(lane == head, jnp.sum(product, axis=1, keepdims=True), dots)
    dot_ref[...] = dots.T
    line = lax.broadcasted_iota(jnp.int32, (16, rows), 0)
    for step in range(blocks):
        head = lax.rem(place_ref[0] + step, blocks)
        side = jnp.zeros((16, rows), jnp.float32)
        for index, term in enumerate(split_three(dot_ref[pl.ds(head, 1), :])):
            side = jnp.where(line == index, term, side)
        outs[step][2 * rows :] = side.astype(jnp.bfloat16)
    for copy in copies:
        copy.wait()


def times(left, right, left_dim, right_dim):
    return lax.dot_general(
        left,
        right,
        (((left_dim,), (right_dim,)), ((), ())),
        preferred_element_type=jnp.float32,
    )


def side_of(pack_ref):
    rows = (pack_ref.shape[0] - 16) // 2
    side = pack_ref[2 * rows :].astype(jnp.float32)
    return side[0:1] + side[1:2] + side[2:3], side[3:4]


def part_of(pack_ref, index):
    rows = (pack_ref.shape[0] - 16) // 2
    return pack_ref[index * rows : (index + 1) * rows]


def weigh_kernel(blocks, place_ref, *refs):
    packs, weight_ref = refs[:blocks], refs[blocks]
    rows = weight_ref.shape[2]
    half = rows // 2
    scale_factor = 1.0 / math.sqrt(packs[0].shape[1])
    local_down = lax.broadcasted_iota(jnp.int32, (rows, 1), 0)
    local_across = lax.broadcasted_iota(jnp.int32, (1, rows), 1)
    line = lax.broadcasted_iota(jnp.int32, (8, rows), 0)
    block_of = [lax.rem(place_ref[0] + step, blocks) for step in range(blocks)]

    def positions(local, block):
        lower = block * half + local
        upper = (2 * blocks - 1 - block) * half + local - half
        return jnp.where(local < half, lower, upper)

    for step in range(blocks):
        mass, docs = side_of(packs[step])
        down = jnp.where(line == 0, mass, docs).T
        mass, docs = down[:, 0:1], down[:, 1:2]
        own_pos = positions(local_down, block_of[step])
        scored = []
        for far in range(2):
            other = (step + 1 + far) % blocks
            score = times(part_of(packs[step], 0), part_of(packs[other], 1), 1, 1) * scale_factor
            allowed = (positions(local_across, block_of[other]) <= own_pos) & (
                side_of(packs[other])[1] == docs
            )
            scored.append(jnp.where(allowed, score, -jnp.inf))
        peak = mass
        for score in scored:
            peak = jnp.maximum(peak, jnp.max(score, axis=1, keepdims=True))
        shifted = [jnp.exp(score - peak) for score in scored]
        total = jnp.exp(mass - peak)
        for part in shifted:
            total = total + jnp.sum(part, axis=1, keepdims=True)
        inverse = 1.0 / total
        for far in range(2):
            weight_ref[step, far] = shifted[far] * inverse


def value_kernel(blocks, place_ref, weight_ref, *refs):
    late, outs = refs[:blocks], refs[blocks:]
    for step in range(blocks):
        near, far = (step - 1) % blocks, (step - 2) % blocks
        value_step = times(
            weight_ref[near, 0].astype(jnp.bfloat16), part_of(late[near], 1), 0, 0
        ) + times(weight_ref[far, 1].astype(jnp.bfloat16), part_of(late[far], 1), 0, 0)
        outs[step][...] = value_step.astype(jnp.bfloat16)


def slope_kernel(blocks, place_ref, weight_ref, *refs):
    packs, late, key_outs, query_outs = (refs[n * blocks : (n + 1) * blocks] for n in range(4))
    slope_ref = refs[4 * blocks]
    rows = weight_ref.shape[2]
    scale_factor = 1.0 / math.sqrt(packs[0].shape[1])
    line = lax.broadcasted_iota(jnp.int32, (8, rows), 0)
    for step in range(blocks):
        row_dot = jnp.where(line == 0, side_of(late[step])[0], 0.0).T[:, 0:1]
        query_step = None
        for far in range(2):
            other = (step + 1 + far) % blocks
            grad_attention = times(part_of(late[step], 1), part_of(late[other], 0), 1, 1)
            slope = weight_ref[step, far] * (grad_attention - row_dot) * scale_factor
            slope = slope.astype(jnp.bfloat16)
            slope_ref[step, far] = slope
            part = times(slope, part_of(packs[other], 1), 1, 0)
            query_step = part if query_step is None else query_step + part
        query_outs[step][...] = query_step.astype(jnp.bfloat16)
    for step in range(blocks):
        near, far = (step - 1) % blocks, (step - 2) % blocks
        key_step = times(slope_ref[near, 0], part_of(packs[near], 0), 0, 0) + times(
            slope_ref[far, 1], part_of(packs[far], 0), 0, 0
        )
        key_outs[step][...] = key_step.astype(jnp.bfloat16)


def gather_kernel(blocks, place_ref, *refs):
    parts = refs[:blocks]
    earlier = refs[blocks]
    outs = refs[blocks + 1 :]
    head_size = parts[0].shape[1]
    for index in range(blocks):
        head = lax.bitwise_xor(place_ref[1], index)
        source = lax.rem(place_ref[0] - head + blocks, blocks)
        columns = pl.ds(pl.multiple_of(head * head_size, head_size), head_size)
        for step in range(blocks):

            @pl.when(source == step)
            def add(step=step, index=index, columns=columns):
                total = earlier[0, :, columns] + parts[step][...].astype(jnp.float32)
                outs[index][...] = total.astype(jnp.bfloat16)


def weight_kernel(blocks, place_ref, own_ref, beside_ref, below_ref, upper_ref, lower_ref, *refs):
    rights = refs[:blocks]
    keep_ref, send_ref = refs[blocks:]
    features, width = keep_ref.shape
    chunk = features // blocks
    core = place_ref[2]
    for index in range(blocks):
        where = slice(index * chunk, (index + 1) * chunk)
        if index < blocks // 2:
            across = upper_ref[where]
        else:
            across = lower_ref[(index - blocks // 2) * chunk : (index - blocks // 2 + 1) * chunk]
        total = None
        for left, right in zip((own_ref[where], beside_ref[where], below_ref[where], across), rights):
            part = jnp.dot(left, right[...], preferred_element_type=jnp.float32)
            total = part if total is None else total + part
        first, second = total[:, :width], total[:, width:]
        keep_ref[where] = jnp.where(core == 0, first, second).astype(jnp.bfloat16)
        send_ref[where] = jnp.where(core == 0, second, first).astype(jnp.bfloat16)


def turn_kernel(place_ref, input_ref, out_ref):
    out_ref[...] = input_ref[0].T


def factor_kernel(place_ref, factor_ref, out_ref):
    total = jnp.sum(factor_ref[...], axis=1, keepdims=True)
    out_ref[...] = jnp.broadcast_to(total, out_ref.shape)


def output_kernel(blocks, place_ref, context_ref, grad_ref, keep_ref, send_ref):
    features, width = keep_ref.shape[1:]
    chunk = features // blocks
    core = place_ref[2]
    for index in range(blocks):
        where = slice(index * chunk, (index + 1) * chunk)
        total = times(grad_ref[0, :, where], context_ref[0], 0, 0)
        for chip in range(blocks):
            first = total[:, 2 * chip * width : (2 * chip + 1) * width]
            second = total[:, (2 * chip + 1) * width : (2 * chip + 2) * width]
            keep_ref[chip, where] = jnp.where(core == 0, first, second).astype(jnp.bfloat16)
            send_ref[chip, where] = jnp.where(core == 0, second, first).astype(jnp.bfloat16)


def pair_kernel(place_ref, keep_ref, other_ref, *outs):
    for index, out in enumerate(outs):
        chip = lax.bitwise_xor(place_ref[1], index)
        total = keep_ref[chip].astype(jnp.float32) + other_ref[chip].astype(jnp.float32)
        out[...] = total.astype(jnp.bfloat16)


def near_kernel(place_ref, *refs):
    parts = refs[:-2]
    keep_ref, send_ref = refs[-2:]
    chunk = keep_ref.shape[1]
    side = lax.bitwise_and(place_ref[0], 1)
    for index in range(2):
        for ref, parity in ((keep_ref, side), (send_ref, 1 - side)):
            where = pl.ds(pl.multiple_of((2 * index + parity) * chunk, chunk), chunk)
            total = parts[0][where].astype(jnp.float32)
            for part in parts[1:]:
                total = total + part[where].astype(jnp.float32)
            ref[index] = total.astype(ref.dtype)


def far_kernel(place_ref, held_ref, other_ref, keep_ref, send_ref):
    side = lax.div(place_ref[0], 2)
    keep_ref[...] = held_ref[side] + other_ref[side].astype(jnp.float32)
    total = held_ref[1 - side] + other_ref[1 - side].astype(jnp.float32)
    send_ref[...] = total.astype(jnp.bfloat16)


def head_body(
    layer_input,
    queries,
    key_rows,
    value_rows,
    context,
    grad_context,
    grad_output,
    earlier_mass,
    grad_queries,
    grad_keys,
    grad_values,
    documents,
    weights,
    row_factor,
    column_factor,
):
    blocks = lax.axis_size("blk")
    data_count = lax.axis_size("dp")
    block = lax.axis_index("blk")
    data = lax.axis_index("dp")
    core = data % 2
    chip = data // 2
    rows = queries.shape[1]
    units = queries.shape[2]
    features = layer_input.shape[2]
    head_size = units // blocks
    width = units // data_count
    vmem = pl.BlockSpec(memory_space=pltpu.VMEM)
    smem = pl.BlockSpec(memory_space=pltpu.SMEM)
    place = jnp.stack([block, chip, core])

    def call(kernel, shapes, *arrays, scratch=(), read=vmem, mib=4):
        return pl.pallas_call(
            kernel,
            out_shape=shapes,
            in_specs=[smem] + [read] * len(arrays),
            out_specs=[vmem] * len(shapes),
            scratch_shapes=list(scratch),
            compiler_params=pltpu.CompilerParams(vmem_limit_bytes=mib * 2**20),
        )(place, *arrays)

    def low(*shape):
        return jax.ShapeDtypeStruct(shape, jnp.bfloat16)

    def heads_moved(kernel, arrays, scratch, mib):
        sent = call(
            lambda *refs: kernel(blocks, *refs),
            [low(2 * rows + 16, head_size)] * blocks,
            *arrays,
            scratch=scratch + [pltpu.SemaphoreType.DMA((2 * blocks + 2,))],
            read=pl.BlockSpec(memory_space=pltpu.HBM),
            mib=mib,
        )
        moved = [sent[0]] + [None] * (blocks - 1)
        for step in range(1, blocks):
            moved[blocks - step] = rotated(sent[step], step)
        return moved

    early = heads_moved(
        pack_early_kernel,
        (queries, key_rows, earlier_mass, documents),
        [
            pltpu.VMEM(earlier_mass.shape, jnp.float32),
            pltpu.VMEM(documents.shape, jnp.int32),
        ],
        58,
    )
    late = heads_moved(
        pack_late_kernel,
        (value_rows, grad_context, context),
        [pltpu.VMEM((1, rows, units), jnp.bfloat16)] * 2 + [pltpu.VMEM((128, rows), jnp.float32)],
        12,
    )

    (turned,) = call(turn_kernel, [low(features, rows)], layer_input)
    mid = features // 2
    beside, below = swapped(turned, 2), swapped(turned, 4)
    upper = swapped(beside[:mid], 4)
    lower = swapped(below[mid:], 2)

    keep, send = call(
        lambda *refs: output_kernel(blocks, *refs),
        [low(blocks, features, width)] * 2,
        context,
        grad_output,
        mib=16,
    )
    pieces = call(pair_kernel, [low(features, width)] * blocks, keep, swapped(send, 1))
    output_parts = [pieces[0]] + [swapped(pieces[index], 2 * index) for index in range(1, blocks)]

    def halved(*parts):
        chunk = features // blocks
        wide = jax.ShapeDtypeStruct((2, chunk, width), jnp.float32)
        held, sent = call(near_kernel, [wide, low(2, chunk, width)], *parts)
        other = traded(sent, 1)
        narrow = jax.ShapeDtypeStruct((chunk, width), jnp.float32)
        held, sent = call(far_kernel, [narrow, low(chunk, width)], held, other)
        return held, traded(sent, 2)

    (factor_part,) = call(
        factor_kernel, [jax.ShapeDtypeStruct((row_factor.shape[0], width), jnp.float32)], row_factor
    )

    weighed = call(
        lambda *refs: weigh_kernel(blocks, *refs),
        [jax.ShapeDtypeStruct((blocks, 2, rows, rows), jnp.float32)],
        *early,
        mib=12,
    )
    valued = call(
        lambda *refs: value_kernel(blocks, *refs),
        [low(rows, head_size)] * blocks,
        weighed[0],
        *late,
        mib=12,
    )
    sloped = call(
        lambda *refs: slope_kernel(blocks, *refs),
        [low(rows, head_size)] * (2 * blocks),
        weighed[0],
        *early,
        *late,
        scratch=[pltpu.VMEM((blocks, 2, rows, rows), jnp.bfloat16)],
        mib=12,
    )
    steps = list(valued) + list(sloped)
    totals = {"o": halved(*output_parts)}
    for g, (name, earlier) in enumerate(
        (("v", grad_values), ("k", grad_keys), ("q", grad_queries))
    ):
        made = steps[g * blocks : (g + 1) * blocks]
        parts = [made[0]] + [rotated(made[step], step) for step in range(1, blocks)]
        rights = call(
            lambda *refs: gather_kernel(blocks, *refs),
            [low(rows, head_size)] * blocks,
            *parts,
            earlier,
        )
        rights = [rights[0]] + [swapped(rights[index], 2 * index) for index in range(1, blocks)]
        keep, send = call(
            lambda *refs: weight_kernel(blocks, *refs),
            [low(features, width)] * 2,
            turned,
            beside,
            below,
            upper,
            lower,
            *rights,
        )
        other = swapped(send, 1)
        totals[name] = halved(keep, other)
    totals = {
        name: sum(part.astype(jnp.float32) for part in parts) for name, parts in totals.items()
    }
    all_tokens = data_count * blocks * rows
    gradient = jnp.stack([totals[name] for name in "qkvo"]) / all_tokens
    return factored_update(
        gradient, weights, row_factor, column_factor, factor_part, blocks, data_count
    )


def factored_update(
    gradient, weights, row_factor, column_factor, factor_part, blocks, data_count
):
    matrices = gradient.shape[0]
    full_rows = gradient.shape[1] * blocks
    full_cols = gradient.shape[2] * data_count
    lanes = gradient.shape[2]
    squares = gradient * gradient + tiny_square
    row_part = jnp.sum(squares, axis=2)
    sent = jnp.concatenate([jnp.sum(squares, axis=1), factor_part], axis=1)
    along = sent
    for step in range(1, blocks):
        along = along + rotated(sent, step)
    col_sum, factor_sum = along[:, :lanes], along[:, lanes]
    new_column_factor = beta_two * column_factor + (1.0 - beta_two) * col_sum / full_rows
    both = jnp.broadcast_to(jnp.sum(col_sum, axis=1, keepdims=True), (matrices, lanes))
    both = jnp.concatenate([row_part, both], axis=1)
    chips = both
    for m in range(2, data_count, 2):
        chips = chips + swapped(both, m)
    chips = chips + swapped(chips, 1)
    row_sum, all_sum = chips[:, :-lanes], chips[:, -1]
    new_row_factor = beta_two * row_factor + (1.0 - beta_two) * row_sum / full_cols
    row_mean = (beta_two * factor_sum + (1.0 - beta_two) * all_sum / full_cols) / full_rows
    second = new_row_factor[:, :, None] * new_column_factor[:, None, :] / row_mean[:, None, None]
    new_weights = weights - learn_rate * gradient * lax.rsqrt(second)
    return (new_weights, new_row_factor, new_column_factor)


def chosen_body(*arrays):
    blocks = lax.axis_size("blk")
    data_count = lax.axis_size("dp")
    heads = arrays[7].shape[1]
    rows, units = arrays[1].shape[1:]
    head_size = units // heads
    if heads == blocks == 4 and data_count == 2 * blocks and rows == head_size and rows % 128 == 0:
        return head_body(*arrays)
    return ring_body(*arrays)


def solution(mesh):
    placed = (
        P("dp", "blk", None),
        P("dp", "blk", None),
        P("dp", "blk", None),
        P("dp", "blk", None),
        P("dp", "blk", None),
        P("dp", "blk", None),
        P("dp", "blk", None),
        P("dp", None, "blk"),
        P("dp", "blk", None),
        P("dp", "blk", None),
        P("dp", "blk", None),
        P("dp", "blk"),
        P(None, "blk", "dp"),
        P(None, "blk"),
        P(None, "dp"),
    )
    return jax.shard_map(
        chosen_body,
        mesh=mesh,
        in_specs=placed,
        out_specs=(P(None, "blk", "dp"), P(None, "blk"), P(None, "dp")),
        check_vma=False,
    )
```

```python
import math

import jax
import jax.numpy as jnp
from jax import lax
from jax.experimental import pallas as pl
from jax.experimental.pallas import tpu as pltpu
from jax.sharding import PartitionSpec as P


beta_two = 0.9
learn_rate = 0.05
tiny_square = 1e-30


def passed_along(value, axis, steps):
    count = lax.axis_size(axis)
    pairs = [(source, (source + steps) % count) for source in range(count)]
    return lax.ppermute(value, axis, pairs)


def as_sent(array):
    return jax.tree.map(lambda a: a.astype(jnp.bfloat16) if a.dtype == jnp.float32 else a, array)


def folded_rows(block_index, blocks, row_count):
    half = row_count // 2
    local = jnp.arange(row_count, dtype=jnp.int32)
    lower = block_index * half + local
    upper = (2 * blocks - 1 - block_index) * half + local - half
    return jnp.where(local < half, lower, upper)


def attend_back(queries, key_rows, value_rows, context, grad_context, earlier_mass, allowed):
    row_count = queries.shape[0]
    key_count = key_rows.shape[0]
    head_count = earlier_mass.shape[0]
    head_size = queries.shape[1] // head_count
    scale_factor = 1.0 / math.sqrt(head_size)
    query_heads = queries.reshape(row_count, head_count, head_size)
    key_heads = key_rows.reshape(key_count, head_count, head_size)
    value_heads = value_rows.reshape(key_count, head_count, head_size)
    context_heads = context.reshape(row_count, head_count, head_size)
    grad_heads = grad_context.reshape(row_count, head_count, head_size)
    scores = (
        jnp.einsum("thd,shd->hts", query_heads, key_heads, preferred_element_type=jnp.float32)
        * scale_factor
    )
    open_pairs = allowed[None]
    peak_score = jnp.maximum(earlier_mass, jnp.max(jnp.where(open_pairs, scores, -jnp.inf), axis=2))
    shifted = jnp.where(open_pairs, jnp.exp(scores - peak_score[:, :, None]), 0.0)
    total_mass = jnp.exp(earlier_mass - peak_score) + jnp.sum(shifted, axis=2)
    log_norm = peak_score + jnp.log(total_mass)
    attention = jnp.where(open_pairs, jnp.exp(scores - log_norm[:, :, None]), 0.0)
    attention_low = attention.astype(jnp.bfloat16)
    row_dot = jnp.sum(context_heads.astype(jnp.float32) * grad_heads.astype(jnp.float32), axis=2).T
    grad_attention = jnp.einsum(
        "thd,shd->hts", grad_heads, value_heads, preferred_element_type=jnp.float32
    )
    grad_scores = (attention * (grad_attention - row_dot[:, :, None]) * scale_factor).astype(
        jnp.bfloat16
    )
    query_step = jnp.einsum(
        "hts,shd->thd", grad_scores, key_heads, preferred_element_type=jnp.float32
    ).reshape(row_count, -1)
    key_step = jnp.einsum(
        "hts,thd->shd", grad_scores, query_heads, preferred_element_type=jnp.float32
    ).reshape(key_count, -1)
    value_step = jnp.einsum(
        "hts,thd->shd", attention_low, grad_heads, preferred_element_type=jnp.float32
    ).reshape(key_count, -1)
    return (query_step, key_step, value_step)


def ring_body(
    layer_input,
    queries,
    key_rows,
    value_rows,
    context,
    grad_context,
    grad_output,
    earlier_mass,
    grad_queries,
    grad_keys,
    grad_values,
    documents,
    weights,
    row_factor,
    column_factor,
):
    blocks = lax.axis_size("blk")
    data_count = lax.axis_size("dp")
    block_index = lax.axis_index("blk")
    row_count = queries.shape[1]
    own_docs = documents[0]
    doc_float = own_docs.astype(jnp.bfloat16)

    def fetch_next(held):
        return passed_along((held[0], held[1], held[2]), "blk", -1)

    nearer = fetch_next((key_rows[0], value_rows[0], doc_float))
    further = fetch_next(nearer)
    seen_keys = jnp.concatenate([nearer[0], further[0]], axis=0)
    seen_values = jnp.concatenate([nearer[1], further[1]], axis=0)
    seen_docs = jnp.concatenate([nearer[2], further[2]], axis=0).astype(jnp.int32)
    own_pos = folded_rows(block_index, blocks, row_count)
    near_pos = folded_rows((block_index + 1) % blocks, blocks, row_count)
    far_pos = folded_rows((block_index + 2) % blocks, blocks, row_count)
    seen_pos = jnp.concatenate([near_pos, far_pos], axis=0)
    allowed = (seen_pos[None, :] <= own_pos[:, None]) & (seen_docs[None, :] == own_docs[:, None])
    query_step, key_step, value_step = attend_back(
        queries[0], seen_keys, seen_values, context[0], grad_context[0], earlier_mass[0], allowed
    )
    near_part = (key_step[:row_count], value_step[:row_count])
    far_part = (key_step[row_count:], value_step[row_count:])

    def send_back(pair):
        return passed_along((as_sent(pair[0]), as_sent(pair[1])), "blk", 1)

    moved = send_back(far_part)
    home = send_back((moved[0] + near_part[0], moved[1] + near_part[1]))
    query_total = grad_queries[0] + query_step
    key_total = grad_keys[0] + home[0]
    value_total = grad_values[0] + home[1]
    right_low = jnp.stack([query_total, key_total, value_total], axis=1).astype(jnp.bfloat16)
    layer_rows = layer_input[0]
    output_rows = grad_output[0]
    context_rows = context[0]
    all_tokens = data_count * blocks * row_count
    part_inner = jnp.einsum(
        "twh,td->hwd", right_low, layer_rows, preferred_element_type=jnp.float32
    )
    part_output = jnp.einsum(
        "th,td->hd", context_rows, output_rows, preferred_element_type=jnp.float32
    )
    summed = lax.psum_scatter(
        jnp.concatenate([part_inner, part_output[:, None, :]], axis=1).astype(jnp.bfloat16),
        "dp",
        scatter_dimension=0,
        tiled=True,
    )
    grouped = lax.psum_scatter(summed, "blk", scatter_dimension=2, tiled=True).astype(jnp.float32)
    gradient = jnp.transpose(grouped, (1, 2, 0)) / all_tokens
    local_rows = gradient.shape[1]
    local_cols = gradient.shape[2]
    full_rows = local_rows * blocks
    full_cols = local_cols * data_count
    squares = gradient * gradient + tiny_square
    row_part = jnp.sum(squares, axis=2)
    col_part = jnp.sum(squares, axis=1)
    row_sum = lax.psum(row_part, "dp")
    col_sum = lax.psum(col_part, "blk")
    new_row_factor = beta_two * row_factor + (1.0 - beta_two) * row_sum / full_cols
    new_column_factor = beta_two * column_factor + (1.0 - beta_two) * col_sum / full_rows
    row_mean = lax.psum(jnp.sum(new_row_factor, axis=1), "blk") / full_rows
    second = new_row_factor[:, :, None] * new_column_factor[:, None, :] / row_mean[:, None, None]
    new_weights = weights - learn_rate * gradient * lax.rsqrt(second)
    return (new_weights, new_row_factor, new_column_factor)


def swapped(value, mask):
    count = lax.axis_size("dp")
    return lax.ppermute(value, "dp", [(source, source ^ mask) for source in range(count)])


def rotated(value, steps):
    count = lax.axis_size("blk")
    pairs = [(source, (source + steps) % count) for source in range(count)]
    return lax.ppermute(value, "blk", pairs)


def traded(value, mask):
    count = lax.axis_size("blk")
    return lax.ppermute(value, "blk", [(source, source ^ mask) for source in range(count)])


def split_three(value):
    high = value.astype(jnp.bfloat16).astype(jnp.float32)
    middle = (value - high).astype(jnp.bfloat16).astype(jnp.float32)
    return (high, middle, value - high - middle)


def pack_heads(blocks, place_ref, stored, outs, arrived):
    rows = stored[0].shape[1]
    head_size = stored[0].shape[2] // blocks
    copies = []
    for step in range(blocks):
        head = lax.rem(place_ref[0] + step, blocks)
        columns = pl.ds(pl.multiple_of(head * head_size, head_size), head_size)
        for index, ref in enumerate(stored):
            target = outs[step].at[index * rows : (index + 1) * rows]
            copies.append(
                pltpu.make_async_copy(ref.at[0, :, columns], target, arrived.at[len(copies)])
            )
    for copy in copies:
        copy.start()
    return copies


def held_copies(stored, held, arrived, first):
    copies = [
        pltpu.make_async_copy(source, target, arrived.at[first + index])
        for index, (source, target) in enumerate(zip(stored, held))
    ]
    for copy in copies:
        copy.start()
    return copies


def pack_early_kernel(blocks, query_ref, key_ref, mass_ref, docs_ref, *refs):
    outs, held = refs[:blocks], refs[blocks : blocks + 2]
    packed_ref, arrived, left = refs[blocks + 2 :]
    place = (lax.axis_index("blk"),)
    slots = [packed_ref.at[step] for step in range(blocks)]
    small = held_copies((mass_ref, docs_ref), held, arrived, 2 * blocks)
    copies = pack_heads(blocks, place, (query_ref, key_ref), slots, arrived)
    rows = docs_ref.shape[1]
    line = lax.broadcasted_iota(jnp.int32, (16, rows), 0)
    for copy in small:
        copy.wait()
    docs = held[1][...].astype(jnp.float32)
    for step in range(blocks):
        head = lax.rem(place[0] + step, blocks)
        side = jnp.where(line == 3, docs, 0.0)
        for index, term in enumerate(split_three(held[0][0, pl.ds(head, 1), :])):
            side = jnp.where(line == index, term, side)
        packed_ref[step, 2 * rows :] = side.astype(jnp.bfloat16)
    leaving = []
    for step in [*range(1, blocks), 0]:
        for copy in copies[2 * step : 2 * step + 2]:
            copy.wait()
        leaving.append(pltpu.make_async_copy(packed_ref.at[step], outs[step], left.at[step]))
        leaving[-1].start()
    for copy in leaving:
        copy.wait()


def pack_late_kernel(blocks, place_ref, value_ref, grad_ref, context_ref, *refs):
    outs, held = refs[:blocks], refs[blocks : blocks + 2]
    dot_ref, arrived = refs[blocks + 2 :]
    large = held_copies((grad_ref, context_ref), held, arrived, 2 * blocks)
    copies = pack_heads(blocks, place_ref, (value_ref, grad_ref), outs, arrived)
    rows = value_ref.shape[1]
    head_size = value_ref.shape[2] // blocks
    for copy in large:
        copy.wait()
    lane = lax.broadcasted_iota(jnp.int32, (rows, 128), 1)
    dots = jnp.zeros((rows, 128), jnp.float32)
    for head in range(blocks):
        columns = slice(head * head_size, (head + 1) * head_size)
        product = held[0][0, :, columns].astype(jnp.float32) * held[1][0, :, columns].astype(
            jnp.float32
        )
        dots = jnp.where(lane == head, jnp.sum(product, axis=1, keepdims=True), dots)
    dot_ref[...] = dots.T
    line = lax.broadcasted_iota(jnp.int32, (16, rows), 0)
    for step in range(blocks):
        head = lax.rem(place_ref[0] + step, blocks)
        side = jnp.zeros((16, rows), jnp.float32)
        for index, term in enumerate(split_three(dot_ref[pl.ds(head, 1), :])):
            side = jnp.where(line == index, term, side)
        outs[step][2 * rows :] = side.astype(jnp.bfloat16)
    for copy in copies:
        copy.wait()


def times(left, right, left_dim, right_dim):
    return lax.dot_general(
        left,
        right,
        (((left_dim,), (right_dim,)), ((), ())),
        preferred_element_type=jnp.float32,
    )


def side_of(pack_ref):
    rows = (pack_ref.shape[0] - 16) // 2
    side = pack_ref[2 * rows :].astype(jnp.float32)
    return side[0:1] + side[1:2] + side[2:3], side[3:4]


def part_of(pack_ref, index):
    rows = (pack_ref.shape[0] - 16) // 2
    return pack_ref[index * rows : (index + 1) * rows]


def weigh_kernel(blocks, place_ref, *refs):
    packs, weight_ref = refs[:blocks], refs[blocks]
    rows = weight_ref.shape[2]
    half = rows // 2
    scale_factor = 1.0 / math.sqrt(packs[0].shape[1])
    local_down = lax.broadcasted_iota(jnp.int32, (rows, 1), 0)
    local_across = lax.broadcasted_iota(jnp.int32, (1, rows), 1)
    line = lax.broadcasted_iota(jnp.int32, (8, rows), 0)
    block_of = [lax.rem(place_ref[0] + step, blocks) for step in range(blocks)]

    def positions(local, block):
        lower = block * half + local
        upper = (2 * blocks - 1 - block) * half + local - half
        return jnp.where(local < half, lower, upper)

    for step in range(blocks):
        mass, docs = side_of(packs[step])
        down = jnp.where(line == 0, mass, docs).T
        mass, docs = down[:, 0:1], down[:, 1:2]
        own_pos = positions(local_down, block_of[step])
        scored = []
        for far in range(2):
            other = (step + 1 + far) % blocks
            score = times(part_of(packs[step], 0), part_of(packs[other], 1), 1, 1) * scale_factor
            allowed = (positions(local_across, block_of[other]) <= own_pos) & (
                side_of(packs[other])[1] == docs
            )
            scored.append(jnp.where(allowed, score, -jnp.inf))
        peak = mass
        for score in scored:
            peak = jnp.maximum(peak, jnp.max(score, axis=1, keepdims=True))
        shifted = [jnp.exp(score - peak) for score in scored]
        total = jnp.exp(mass - peak)
        for part in shifted:
            total = total + jnp.sum(part, axis=1, keepdims=True)
        inverse = 1.0 / total
        for far in range(2):
            weight_ref[step, far] = shifted[far] * inverse


def value_kernel(blocks, place_ref, weight_ref, *refs):
    late, outs = refs[:blocks], refs[blocks:]
    for step in range(blocks):
        near, far = (step - 1) % blocks, (step - 2) % blocks
        value_step = times(
            weight_ref[near, 0].astype(jnp.bfloat16), part_of(late[near], 1), 0, 0
        ) + times(weight_ref[far, 1].astype(jnp.bfloat16), part_of(late[far], 1), 0, 0)
        outs[step][...] = value_step.astype(jnp.bfloat16)


def slope_kernel(blocks, place_ref, weight_ref, *refs):
    packs, late, key_outs, query_outs = (refs[n * blocks : (n + 1) * blocks] for n in range(4))
    slope_ref = refs[4 * blocks]
    rows = weight_ref.shape[2]
    scale_factor = 1.0 / math.sqrt(packs[0].shape[1])
    line = lax.broadcasted_iota(jnp.int32, (8, rows), 0)
    for step in range(blocks):
        row_dot = jnp.where(line == 0, side_of(late[step])[0], 0.0).T[:, 0:1]
        query_step = None
        for far in range(2):
            other = (step + 1 + far) % blocks
            grad_attention = times(part_of(late[step], 1), part_of(late[other], 0), 1, 1)
            slope = weight_ref[step, far] * (grad_attention - row_dot) * scale_factor
            slope = slope.astype(jnp.bfloat16)
            slope_ref[step, far] = slope
            part = times(slope, part_of(packs[other], 1), 1, 0)
            query_step = part if query_step is None else query_step + part
        query_outs[step][...] = query_step.astype(jnp.bfloat16)
    for step in range(blocks):
        near, far = (step - 1) % blocks, (step - 2) % blocks
        key_step = times(slope_ref[near, 0], part_of(packs[near], 0), 0, 0) + times(
            slope_ref[far, 1], part_of(packs[far], 0), 0, 0
        )
        key_outs[step][...] = key_step.astype(jnp.bfloat16)


def gather_kernel(blocks, place_ref, *refs):
    parts = refs[:blocks]
    earlier = refs[blocks]
    outs = refs[blocks + 1 :]
    head_size = parts[0].shape[1]
    for index in range(blocks):
        head = lax.bitwise_xor(place_ref[1], index)
        source = lax.rem(place_ref[0] - head + blocks, blocks)
        columns = pl.ds(pl.multiple_of(head * head_size, head_size), head_size)
        for step in range(blocks):

            @pl.when(source == step)
            def add(step=step, index=index, columns=columns):
                total = earlier[0, :, columns] + parts[step][...].astype(jnp.float32)
                outs[index][...] = total.astype(jnp.bfloat16)


def weight_kernel(blocks, place_ref, own_ref, beside_ref, below_ref, upper_ref, lower_ref, *refs):
    rights = refs[:blocks]
    keep_ref, send_ref = refs[blocks:]
    features, width = keep_ref.shape
    chunk = features // blocks
    core = place_ref[2]
    for index in range(blocks):
        where = slice(index * chunk, (index + 1) * chunk)
        if index < blocks // 2:
            across = upper_ref[where]
        else:
            across = lower_ref[(index - blocks // 2) * chunk : (index - blocks // 2 + 1) * chunk]
        total = None
        for left, right in zip((own_ref[where], beside_ref[where], below_ref[where], across), rights):
            part = jnp.dot(left, right[...], preferred_element_type=jnp.float32)
            total = part if total is None else total + part
        first, second = total[:, :width], total[:, width:]
        keep_ref[where] = jnp.where(core == 0, first, second).astype(jnp.bfloat16)
        send_ref[where] = jnp.where(core == 0, second, first).astype(jnp.bfloat16)


def turn_kernel(place_ref, input_ref, out_ref):
    out_ref[...] = input_ref[0].T


def factor_kernel(place_ref, factor_ref, out_ref):
    total = jnp.sum(factor_ref[...], axis=1, keepdims=True)
    out_ref[...] = jnp.broadcast_to(total, out_ref.shape)


def output_kernel(blocks, place_ref, context_ref, grad_ref, keep_ref, send_ref):
    features, width = keep_ref.shape[1:]
    chunk = features // blocks
    core = place_ref[2]
    for index in range(blocks):
        where = slice(index * chunk, (index + 1) * chunk)
        total = times(grad_ref[0, :, where], context_ref[0], 0, 0)
        for chip in range(blocks):
            first = total[:, 2 * chip * width : (2 * chip + 1) * width]
            second = total[:, (2 * chip + 1) * width : (2 * chip + 2) * width]
            keep_ref[chip, where] = jnp.where(core == 0, first, second).astype(jnp.bfloat16)
            send_ref[chip, where] = jnp.where(core == 0, second, first).astype(jnp.bfloat16)


def pair_kernel(place_ref, keep_ref, other_ref, *outs):
    for index, out in enumerate(outs):
        chip = lax.bitwise_xor(place_ref[1], index)
        total = keep_ref[chip].astype(jnp.float32) + other_ref[chip].astype(jnp.float32)
        out[...] = total.astype(jnp.bfloat16)


def near_kernel(place_ref, *refs):
    parts = refs[:-2]
    keep_ref, send_ref = refs[-2:]
    chunk = keep_ref.shape[1]
    side = lax.bitwise_and(place_ref[0], 1)
    for index in range(2):
        for ref, parity in ((keep_ref, side), (send_ref, 1 - side)):
            where = pl.ds(pl.multiple_of((2 * index + parity) * chunk, chunk), chunk)
            total = parts[0][where].astype(jnp.float32)
            for part in parts[1:]:
                total = total + part[where].astype(jnp.float32)
            ref[index] = total.astype(ref.dtype)


def far_kernel(place_ref, held_ref, other_ref, keep_ref, send_ref):
    side = lax.div(place_ref[0], 2)
    keep_ref[...] = held_ref[side] + other_ref[side].astype(jnp.float32)
    total = held_ref[1 - side] + other_ref[1 - side].astype(jnp.float32)
    send_ref[...] = total.astype(jnp.bfloat16)


def head_body(
    layer_input,
    queries,
    key_rows,
    value_rows,
    context,
    grad_context,
    grad_output,
    earlier_mass,
    grad_queries,
    grad_keys,
    grad_values,
    documents,
    weights,
    row_factor,
    column_factor,
):
    blocks = lax.axis_size("blk")
    data_count = lax.axis_size("dp")
    block = lax.axis_index("blk")
    data = lax.axis_index("dp")
    core = data % 2
    chip = data // 2
    rows = queries.shape[1]
    units = queries.shape[2]
    features = layer_input.shape[2]
    head_size = units // blocks
    width = units // data_count
    vmem = pl.BlockSpec(memory_space=pltpu.VMEM)
    smem = pl.BlockSpec(memory_space=pltpu.SMEM)
    place = jnp.stack([block, chip, core])

    def call(kernel, shapes, *arrays, scratch=(), read=vmem, mib=4, placed=True):
        made = pl.pallas_call(
            kernel,
            out_shape=shapes,
            in_specs=[smem] * placed + [read] * len(arrays),
            out_specs=[vmem if placed else read] * len(shapes),
            scratch_shapes=list(scratch),
            compiler_params=pltpu.CompilerParams(vmem_limit_bytes=mib * 2**20),
        )
        return made(place, *arrays) if placed else made(*arrays)

    def low(*shape):
        return jax.ShapeDtypeStruct(shape, jnp.bfloat16)

    def heads_moved(kernel, arrays, scratch, mib, placed):
        sent = call(
            lambda *refs: kernel(blocks, *refs),
            [low(2 * rows + 16, head_size)] * blocks,
            *arrays,
            scratch=scratch,
            read=pl.BlockSpec(memory_space=pltpu.HBM),
            mib=mib,
            placed=placed,
        )
        moved = [sent[0]] + [None] * (blocks - 1)
        for step in range(1, blocks):
            moved[blocks - step] = rotated(sent[step], step)
        return moved

    early = heads_moved(
        pack_early_kernel,
        (queries, key_rows, earlier_mass, documents),
        [
            pltpu.VMEM(earlier_mass.shape, jnp.float32),
            pltpu.VMEM(documents.shape, jnp.int32),
            pltpu.VMEM((blocks, 2 * rows + 16, head_size), jnp.bfloat16),
            pltpu.SemaphoreType.DMA((2 * blocks + 2,)),
            pltpu.SemaphoreType.DMA((blocks,)),
        ],
        58,
        False,
    )
    late = heads_moved(
        pack_late_kernel,
        (value_rows, grad_context, context),
        [pltpu.VMEM((1, rows, units), jnp.bfloat16)] * 2
        + [pltpu.VMEM((128, rows), jnp.float32), pltpu.SemaphoreType.DMA((2 * blocks + 2,))],
        12,
        True,
    )

    (turned,) = call(turn_kernel, [low(features, rows)], layer_input)
    mid = features // 2
    beside, below = swapped(turned, 2), swapped(turned, 4)
    upper = swapped(beside[:mid], 4)
    lower = swapped(below[mid:], 2)

    keep, send = call(
        lambda *refs: output_kernel(blocks, *refs),
        [low(blocks, features, width)] * 2,
        context,
        grad_output,
        mib=16,
    )
    pieces = call(pair_kernel, [low(features, width)] * blocks, keep, swapped(send, 1))
    output_parts = [pieces[0]] + [swapped(pieces[index], 2 * index) for index in range(1, blocks)]

    def halved(*parts):
        chunk = features // blocks
        wide = jax.ShapeDtypeStruct((2, chunk, width), jnp.float32)
        held, sent = call(near_kernel, [wide, low(2, chunk, width)], *parts)
        other = traded(sent, 1)
        narrow = jax.ShapeDtypeStruct((chunk, width), jnp.float32)
        held, sent = call(far_kernel, [narrow, low(chunk, width)], held, other)
        return held, traded(sent, 2)

    (factor_part,) = call(
        factor_kernel, [jax.ShapeDtypeStruct((row_factor.shape[0], width), jnp.float32)], row_factor
    )

    weighed = call(
        lambda *refs: weigh_kernel(blocks, *refs),
        [jax.ShapeDtypeStruct((blocks, 2, rows, rows), jnp.float32)],
        *early,
        mib=12,
    )
    valued = call(
        lambda *refs: value_kernel(blocks, *refs),
        [low(rows, head_size)] * blocks,
        weighed[0],
        *late,
        mib=12,
    )
    sloped = call(
        lambda *refs: slope_kernel(blocks, *refs),
        [low(rows, head_size)] * (2 * blocks),
        weighed[0],
        *early,
        *late,
        scratch=[pltpu.VMEM((blocks, 2, rows, rows), jnp.bfloat16)],
        mib=12,
    )
    steps = list(valued) + list(sloped)
    totals = {"o": halved(*output_parts)}
    for g, (name, earlier) in enumerate(
        (("v", grad_values), ("k", grad_keys), ("q", grad_queries))
    ):
        made = steps[g * blocks : (g + 1) * blocks]
        parts = [made[0]] + [rotated(made[step], step) for step in range(1, blocks)]
        rights = call(
            lambda *refs: gather_kernel(blocks, *refs),
            [low(rows, head_size)] * blocks,
            *parts,
            earlier,
        )
        rights = [rights[0]] + [swapped(rights[index], 2 * index) for index in range(1, blocks)]
        keep, send = call(
            lambda *refs: weight_kernel(blocks, *refs),
            [low(features, width)] * 2,
            turned,
            beside,
            below,
            upper,
            lower,
            *rights,
        )
        other = swapped(send, 1)
        totals[name] = halved(keep, other)
    totals = {
        name: sum(part.astype(jnp.float32) for part in parts) for name, parts in totals.items()
    }
    all_tokens = data_count * blocks * rows
    gradient = jnp.stack([totals[name] for name in "qkvo"]) / all_tokens
    return factored_update(
        gradient, weights, row_factor, column_factor, factor_part, blocks, data_count
    )


def factored_update(
    gradient, weights, row_factor, column_factor, factor_part, blocks, data_count
):
    matrices = gradient.shape[0]
    full_rows = gradient.shape[1] * blocks
    full_cols = gradient.shape[2] * data_count
    lanes = gradient.shape[2]
    squares = gradient * gradient + tiny_square
    row_part = jnp.sum(squares, axis=2)
    sent = jnp.concatenate([jnp.sum(squares, axis=1), factor_part], axis=1)
    along = sent
    for step in range(1, blocks):
        along = along + rotated(sent, step)
    col_sum, factor_sum = along[:, :lanes], along[:, lanes]
    new_column_factor = beta_two * column_factor + (1.0 - beta_two) * col_sum / full_rows
    both = jnp.broadcast_to(jnp.sum(col_sum, axis=1, keepdims=True), (matrices, lanes))
    both = jnp.concatenate([row_part, both], axis=1)
    chips = both
    for m in range(2, data_count, 2):
        chips = chips + swapped(both, m)
    chips = chips + swapped(chips, 1)
    row_sum, all_sum = chips[:, :-lanes], chips[:, -1]
    new_row_factor = beta_two * row_factor + (1.0 - beta_two) * row_sum / full_cols
    row_mean = (beta_two * factor_sum + (1.0 - beta_two) * all_sum / full_cols) / full_rows
    second = new_row_factor[:, :, None] * new_column_factor[:, None, :] / row_mean[:, None, None]
    new_weights = weights - learn_rate * gradient * lax.rsqrt(second)
    return (new_weights, new_row_factor, new_column_factor)


def chosen_body(*arrays):
    blocks = lax.axis_size("blk")
    data_count = lax.axis_size("dp")
    heads = arrays[7].shape[1]
    rows, units = arrays[1].shape[1:]
    head_size = units // heads
    if heads == blocks == 4 and data_count == 2 * blocks and rows == head_size and rows % 128 == 0:
        return head_body(*arrays)
    return ring_body(*arrays)


def solution(mesh):
    placed = (
        P("dp", "blk", None),
        P("dp", "blk", None),
        P("dp", "blk", None),
        P("dp", "blk", None),
        P("dp", "blk", None),
        P("dp", "blk", None),
        P("dp", "blk", None),
        P("dp", None, "blk"),
        P("dp", "blk", None),
        P("dp", "blk", None),
        P("dp", "blk", None),
        P("dp", "blk"),
        P(None, "blk", "dp"),
        P(None, "blk"),
        P(None, "dp"),
    )
    return jax.shard_map(
        chosen_body,
        mesh=mesh,
        in_specs=placed,
        out_specs=(P(None, "blk", "dp"), P(None, "blk"), P(None, "dp")),
        check_vma=False,
    )
```
